32 devices in a mesh: dom: 2 (over y), wide: 16 (over z, x, core).
Axes of the slice: x: 2, y: 2, z: 4, core: 2. Of those that a mesh axis runs over, the one named last changes fastest.
Arguments:
- embeddings: bfloat16 [16384, 768], P(('dom', 'wide')), parts along dimension 0, may hold values from -6 to 6
- cluster_id: int32 [16384, 1], P(('dom', 'wide')), parts along dimension 0, may hold values from 0 to 7; in each aligned block of 512 rows (0 to 511, 512 to 1023, ...) at most 160 rows name the same one
Outputs:
- max_similarity: float32 [16384], P(('dom', 'wide')), parts along dimension 0
The draws below stay inside these ranges and needn't reach their ends.
There are 2 independent parts, one for each index of `dom`. The reference program is written for one: setup_inputs(seed, part) draws one part's arguments, and reference() takes and returns one part's arrays. A program takes and returns all parts, laid end to end along the dimension named above; each array names one. Nothing has to cross between parts.
Inputs may be any that keep to these rules, and one draw needn't show every extreme that they name: `cluster_id`: among the 512 rows of one device (aligned blocks of 512 rows), no cluster appears more than 160 times; every cluster has some row.
All inputs are finite; a program needn't handle non-finite values.
Results may differ from the reference program's by a relative error of at most 0.0014.
Values may be sent and summed in bfloat16 or wider, within the bound.
No kernel may reach another device: no remote copies, remote signals or barrier semaphores. Data moves between devices by JAX's collectives and lax.ppermute only.
A program may use at most 64 MiB of HBM per device.

```python
import math
import jax
import jax.numpy as jnp
import numpy as np
from jax import lax

D = 768
ROW_DEV = 512
CLUSTERS = 8
MOST = 160
ROWS = 8192
N_WIDE = 16


def steps_of(own_key, shape, pieces, smallest, high):
    factor_of, own = 1.0, jax.random.fold_in(own_key, 6)
    for axis_at, parts in pieces:
        steps = jnp.exp(jax.random.uniform(jax.random.fold_in(own, axis_at), (parts,), jnp.float32, smallest / len(pieces), high / len(pieces)))
        factor_of = factor_of * jnp.repeat(steps, shape[axis_at] // parts).reshape([-1 if axis == axis_at else 1 for axis in range(len(shape))])
    return factor_of


def deal_out(stream_key, own, number, rows, count, top, bound, lean):
    ranking = jax.random.permutation(stream_key, count)
    packed, common = portions_of(count, rows * top, bound, lean, True), portions_of(count, rows * top, bound, lean, False)
    places = jnp.arange(count)

    def named(lengths, offset_by):
        used = int((lengths > 0).sum())
        fixed = max(1, used // 4)
        shifted = fixed + (places - fixed + offset_by * (used - fixed)) % max(1, count - fixed)
        return jnp.zeros((count,), jnp.int32).at[ranking[jnp.where(places < fixed, places, shifted)]].set(jnp.asarray(lengths, jnp.int32))

    lengths = jnp.where(number % 4 == 0, named(packed, number // 4), named(common, number - number // 4 - 1))
    mixed = jax.random.permutation(jax.random.fold_in(own, 3), count)
    donor, taker = mixed[0:count // 2 * 2:2], mixed[1:count // 2 * 2:2]
    margin = jnp.minimum(lengths[donor] - 1, bound - lengths[taker]) // 2
    margin = jnp.where((donor == ranking[0]) | (taker == ranking[0]) | (lengths[taker] == 0), 0, jnp.maximum(margin, 0))
    shifted = jax.random.randint(jax.random.fold_in(own, 4), (count // 2,), 0, 1 << 20) % (margin + 1)
    lengths = lengths.at[donor].add(-shifted).at[taker].add(shifted)
    members = jnp.searchsorted(jnp.cumsum(lengths), jnp.arange(rows * top), side="right").astype(jnp.int32)
    listing = members.reshape(top, rows).T
    listing = listing[jax.random.permutation(jax.random.fold_in(own, 1), rows)]
    offset_by = jax.random.randint(jax.random.fold_in(own, 2), (rows, 1), 0, top)
    return jnp.take_along_axis(listing, (jnp.arange(top)[None, :] + offset_by) % top, axis=1)


def portions_of(amount, total, reach, lean, full):
    portions = [(1 << 20) // math.isqrt(standing ** lean) + 1 for standing in range(1, amount + 1)]
    largest = reach if full else min(reach, max(-(-total // amount), total * portions[0] // sum(portions)))
    least = 1 if total - largest >= amount - 1 else 0
    holding, rest = [largest] + [least] * (amount - 1), total - largest - least * (amount - 1)
    while rest > 0:
        candidates = [i for i in range(1, amount) if holding[i] < largest] or [i for i in range(1, amount) if holding[i] < reach]
        whole, remaining = sum([portions[i] for i in candidates]), rest
        for i in candidates:
            extra = min(reach - holding[i], max(1, remaining * portions[i] // whole), rest)
            holding[i] = holding[i] + extra
            rest = rest - extra
    return np.array(holding)


def noise(own_key, extent, width, reach, cuts=(), kind=jnp.bfloat16):
    gain = steps_of(own_key, extent, cuts, -0.22, 0.18) if cuts else 1.0
    entries = jax.random.normal(own_key, extent, jnp.float32) * width * gain
    return jnp.minimum(jnp.maximum(entries, -reach), reach).astype(kind)


def setup_inputs(seed: int = 0, part: int = 0) -> dict:
    key_of = jax.random.split(jax.random.key(seed), 3)
    part_splits = jax.random.split(jax.random.fold_in(key_of[2], part), 3)
    embeddings = noise(part_splits[0], (ROWS, D), 1.0, 6.0, ((0, 16),))
    cluster_id_keys = jax.random.split(jax.random.fold_in(part_splits[1], 1), ROWS // ROW_DEV)
    cluster_id_turns = jax.random.permutation(jax.random.fold_in(part_splits[1], 3), ROWS // ROW_DEV)
    cluster_id = jax.vmap(lambda own, number: deal_out(jax.random.fold_in(part_splits[1], 2), own, number, ROW_DEV, CLUSTERS, 1, MOST, 1))(cluster_id_keys, cluster_id_turns).reshape((ROWS, 1))
    return {"embeddings": embeddings, "cluster_id": cluster_id}


def normalize(embedded):
    values = embedded.astype(jnp.float32)
    inverse = lax.rsqrt(lax.optimization_barrier(jnp.mean(values * values, axis=1, keepdims=True)) + 1e-06)
    return (values * inverse * (1.0 / math.sqrt(values.shape[1]))).astype(jnp.bfloat16)

def reference(embeddings, cluster_id):
    unit_rows = normalize(embeddings).astype(jnp.float32)
    labels = cluster_id[:, 0].astype(jnp.int32)
    sorted_index = jnp.argsort(labels, stable=True).astype(jnp.int32)
    sorted_rows = unit_rows[sorted_index]
    sorted_labels = labels[sorted_index]
    window = MOST * N_WIDE
    feature_dim = unit_rows.shape[1]
    padded_rows = jnp.concatenate([jnp.zeros((window, feature_dim), jnp.float32), sorted_rows], axis=0)
    padded_labels = jnp.concatenate([jnp.full((window,), -1, jnp.int32), sorted_labels], axis=0)
    positions = jnp.arange(ROWS, dtype=jnp.int32)
    padded_positions = jnp.concatenate([jnp.full((window,), -1, jnp.int32), positions], axis=0)

    def block_max(start):
        queries = lax.dynamic_slice_in_dim(sorted_rows, start, ROW_DEV, 0)
        query_labels = lax.dynamic_slice_in_dim(sorted_labels, start, ROW_DEV, 0)
        query_positions = start + jnp.arange(ROW_DEV, dtype=jnp.int32)
        key_rows = lax.dynamic_slice_in_dim(padded_rows, start, window + ROW_DEV, 0)
        key_labels = lax.dynamic_slice_in_dim(padded_labels, start, window + ROW_DEV, 0)
        key_positions = lax.dynamic_slice_in_dim(padded_positions, start, window + ROW_DEV, 0)
        scores = jnp.dot(queries, key_rows.T, precision=lax.Precision.HIGHEST)
        allowed = (key_labels[None, :] == query_labels[:, None]) & (key_positions[None, :] < query_positions[:, None])
        return lax.optimization_barrier(jnp.max(jnp.where(allowed, scores, -1.0), axis=1))
    starts = jnp.arange(N_WIDE, dtype=jnp.int32) * ROW_DEV
    sorted_best = lax.map(block_max, starts).reshape(-1)
    return jnp.zeros((ROWS,), jnp.float32).at[sorted_index].set(sorted_best)
```

```python
import functools
import math

import jax
import jax.numpy as jnp
from jax import lax
from jax.experimental import pallas as pl
from jax.experimental.pallas import tpu as pltpu
from jax.sharding import PartitionSpec as P


def swapped(value, axis, bit):
    mask = 2**bit
    pairs = [(source, source ^ mask) for source in range(lax.axis_size(axis))]
    return lax.ppermute(value, axis, pairs)


def normalize(embedded):
    values = embedded.astype(jnp.float32)
    inverse = lax.rsqrt(jnp.mean(values * values, axis=1, keepdims=True) + 1e-06)
    return (values * inverse * (1.0 / math.sqrt(values.shape[1]))).astype(jnp.bfloat16)


def pair_scores(queries, key_rows):
    return jnp.einsum("qd,kd->qk", queries, key_rows, preferred_element_type=jnp.float32)


def masked_max(scores, allowed):
    return jnp.max(jnp.where(allowed, scores, -1.0), axis=1)


def routed(embeddings, cluster_id):
    axis_size = lax.axis_size("wide")
    rows_dev = embeddings.shape[0]
    feature_dim = embeddings.shape[1]
    clusters = axis_size // 2
    capacity = (5 * rows_dev + 2 * axis_size - 1) // (2 * axis_size)
    buffer_rows = axis_size * capacity
    unit_rows = normalize(embeddings)
    labels = cluster_id[:, 0]
    my_index = lax.axis_index("wide")
    my_flip = my_index % 2
    position = lax.iota(jnp.int32, rows_dev)
    same_cluster = labels[:, None] == labels[None, :]
    earlier = position[None, :] < position[:, None]
    local_rank = jnp.sum((same_cluster & earlier).astype(jnp.int32), axis=1)
    target = 2 * labels + (local_rank + my_flip) % 2
    slot_index = target * capacity + local_rank // 2
    outgoing = jnp.zeros((buffer_rows, feature_dim), jnp.bfloat16).at[slot_index].set(unit_rows)
    cluster_count = jnp.sum(
        (labels[:, None] == lax.iota(jnp.int32, clusters)[None, :]).astype(jnp.int32), axis=0
    )
    parity = lax.iota(jnp.int32, axis_size) % 2
    send_count = (jnp.repeat(cluster_count, 2) + 1 - (parity + my_flip) % 2) // 2
    outgoing_blocks = outgoing.reshape(axis_size, capacity, feature_dim)
    count_blocks = send_count.reshape(axis_size, 1)
    received, counts = (
        lax.all_to_all(outgoing_blocks, "wide", split_axis=0, concat_axis=0, tiled=True),
        lax.all_to_all(count_blocks, "wide", split_axis=0, concat_axis=0, tiled=True),
    )
    own_rows = received.reshape(buffer_rows, feature_dim)
    partner, partner_counts = swapped((own_rows, counts), "wide", 0)
    side_bit = my_index % 2
    slot_pos = lax.iota(jnp.int32, capacity)
    sources = lax.iota(jnp.int32, axis_size)
    base_key = (sources[:, None] * (2 * capacity) + 2 * slot_pos[None, :]).reshape(-1)
    source_parity = jnp.repeat(sources % 2, capacity)
    own_key = base_key + (side_bit + source_parity) % 2
    partner_key = base_key + (1 - side_bit + source_parity) % 2
    own_live = (slot_pos[None, :] < counts).reshape(-1)
    partner_live = (slot_pos[None, :] < partner_counts).reshape(-1)
    blocks = 8
    query_rows = own_rows.reshape(blocks, -1, feature_dim)
    query_key = own_key.reshape(blocks, -1)

    def self_max(pieces):
        queries, keys_here = pieces
        return masked_max(
            pair_scores(queries, own_rows),
            own_live[None, :] & (own_key[None, :] < keys_here[:, None]),
        )

    self_best = lax.map(self_max, (query_rows, query_key)).reshape(-1)
    first = side_bit == 0
    left_rows = jnp.where(first, own_rows, partner)
    left_key = jnp.where(first, own_key, partner_key)
    left_live = jnp.where(first, own_live, partner_live)
    right_rows = jnp.where(first, partner, own_rows)
    right_key = jnp.where(first, partner_key, own_key)
    right_live = jnp.where(first, partner_live, own_live)
    half_rows = buffer_rows // 2
    start = side_bit * half_rows
    lower_rows = lax.dynamic_slice_in_dim(left_rows, start, half_rows, 0).reshape(
        blocks // 2, -1, feature_dim
    )
    lower_key = lax.dynamic_slice_in_dim(left_key, start, half_rows, 0).reshape(blocks // 2, -1)
    lower_live = lax.dynamic_slice_in_dim(left_live, start, half_rows, 0).reshape(blocks // 2, -1)

    def cross_max(pieces):
        queries, keys_here, live_here = pieces
        scores = pair_scores(queries, right_rows)
        row_best = masked_max(
            scores, right_live[None, :] & (right_key[None, :] < keys_here[:, None])
        )
        column_mask = live_here[:, None] & (keys_here[:, None] < right_key[None, :])
        column_best = jnp.max(jnp.where(column_mask, scores, -1.0), axis=0)
        return (row_best, column_best)

    row_best, column_best = lax.map(cross_max, (lower_rows, lower_key, lower_live))
    row_best = row_best.reshape(-1)
    column_best = jnp.max(column_best, axis=0)
    placed = lax.dynamic_update_slice_in_dim(
        jnp.full((buffer_rows,), -1.0, jnp.float32), row_best, start, 0
    )
    kept = jnp.where(first, placed, column_best)
    handed = jnp.where(first, column_best, placed)
    returned = swapped(handed, "wide", 0)
    best_all = jnp.maximum(self_best, jnp.maximum(kept, returned))
    back = lax.all_to_all(
        best_all.reshape(axis_size, capacity), "wide", split_axis=0, concat_axis=0, tiled=True
    )
    return back.reshape(-1)[slot_index]


LAYERS = 4
TAG_ROWS = 16


def tag_kernel(rows_ref, label_ref, out_ref):
    rows, width = rows_ref.shape
    values = rows_ref[...].astype(jnp.float32)
    inverse = lax.rsqrt(jnp.mean(values * values, axis=1, keepdims=True) + 1e-06)
    unit = values * inverse * (1.0 / math.sqrt(width))
    out_ref[:rows, :] = unit.astype(jnp.bfloat16)
    codes = (label_ref[...] + 1).astype(jnp.float32)
    out_ref[rows:, :rows] = jnp.broadcast_to(codes, (TAG_ROWS, rows)).astype(jnp.bfloat16)
    if rows < width:
        out_ref[rows:, rows:] = jnp.zeros((TAG_ROWS, width - rows), jnp.bfloat16)


def tagged(embeddings, labels):
    rows, width = embeddings.shape
    return pl.pallas_call(
        tag_kernel,
        out_shape=jax.ShapeDtypeStruct((rows + TAG_ROWS, width), jnp.bfloat16),
        name="tagged",
    )(embeddings, labels.reshape(1, rows))


def code_row(block_ref):
    rows = block_ref.shape[0] - TAG_ROWS
    return block_ref[rows:, :rows].astype(jnp.float32)[:1]


def best_kernel(tasks, n_keys, n_queries, started, flags_ref, *refs):
    key_refs = refs[:n_keys]
    query_refs = refs[n_keys : n_keys + n_queries]
    begun_ref = refs[n_keys + n_queries] if started else None
    out_ref = refs[-1]
    rows = query_refs[0].shape[0] - TAG_ROWS
    step = rows // 2
    key_codes = []
    for ref in key_refs:
        wide = jnp.broadcast_to(code_row(ref), (128, rows))
        key_codes.append(jnp.transpose(wide))
    for q, query_ref in enumerate(query_refs):
        queries = query_ref[:rows, :]
        row_code = code_row(query_ref)
        best = [None] * (rows // 128)
        for k, mode in tasks[q]:
            code = row_code
            if isinstance(mode, int):
                code = jnp.where(flags_ref[mode] != 0, row_code, -1.0)
            for start in range(0, rows, step):
                scores = lax.dot_general(
                    key_refs[k][start : start + step, :],
                    queries,
                    (((1,), (1,)), ((), ())),
                    preferred_element_type=jnp.float32,
                )
                for b in range(rows // 128):
                    low = b * 128
                    if mode == "before" and start >= low + 128:
                        continue
                    allowed = key_codes[k][start : start + step] == code[:, low : low + 128]
                    if mode == "before":
                        key_at = lax.broadcasted_iota(jnp.int32, (step, 128), 0) + start
                        query_at = lax.broadcasted_iota(jnp.int32, (step, 128), 1) + low
                        allowed = allowed & (key_at < query_at)
                    kept = jnp.where(allowed, scores[:, low : low + 128], -1.0)
                    part = jnp.max(kept.reshape(step // 8, 8, 128), axis=0)
                    best[b] = part if best[b] is None else jnp.maximum(best[b], part)
        for b, part in enumerate(best):
            low = b * 128
            line = jnp.max(part, axis=0, keepdims=True)
            if started:
                line = jnp.maximum(line, begun_ref[q : q + 1, low : low + 128])
            out_ref[q : q + 1, low : low + 128] = line


def best_of(tasks, keys, queries, flags, begun, name):
    rows = queries[0].shape[0] - TAG_ROWS
    arrays = list(keys) + list(queries) + ([] if begun is None else [begun])
    body = functools.partial(best_kernel, tasks, len(keys), len(queries), begun is not None)
    return pl.pallas_call(
        body,
        out_shape=jax.ShapeDtypeStruct((len(queries), rows), jnp.float32),
        in_specs=[pl.BlockSpec(memory_space=pltpu.SMEM)]
        + [pl.BlockSpec(memory_space=pltpu.VMEM)] * len(arrays),
        name=name,
    )(flags, *arrays)


def layered(embeddings, cluster_id):
    mine = tagged(embeddings, cluster_id[:, 0])
    spots = [(z, x, c) for z in range(LAYERS) for x in range(2) for c in range(2)]

    def at(z, x, c):
        return (z * 2 + x) * 2 + c

    def sent(value, hops):
        return lax.ppermute(value, "wide", hops)

    across = [(at(z, x, c), at(z, 1 - x, c)) for z, x, c in spots]
    beside = [(at(z, x, c), at(z, x, 1 - c)) for z, x, c in spots]
    rise = [(at(z, x, c), at(z + 1, x, c)) for z, x, c in spots if z + 1 < LAYERS]
    leap = [(at(z, x, c), at(z + 2, x, c)) for z, x, c in spots if z == 0]
    fall = [(at(z, x, c), at(z - 1, x, c)) for z, x, c in spots if z == LAYERS - 1]
    slant = [(at(z, x, c), at(z - 1, 1 - x, c)) for z, x, c in spots if z == LAYERS - 1]

    below = sent(mine, rise)
    above = sent(mine, fall)
    side = sent(mine, across)
    deep = sent(mine, leap)
    far = sent(mine, slant)
    twin = sent(mine, beside)
    below_twin = sent(below, beside)
    deep_twin = sent(deep, beside)

    my_index = lax.axis_index("wide")
    layer = my_index // 4
    column = (my_index // 2) % 2
    core = my_index % 2
    flags = jnp.stack([core, 1 - column]).astype(jnp.int32)

    near = best_of(
        [[(0, "before"), (1, 0)], [(0, 1), (1, 1)]],
        [mine, twin], [mine, side], flags, None, "near",
    )
    lower = best_of(
        [[(0, "all"), (1, "all")]] * 3,
        [below, below_twin], [mine, side, above], flags,
        jnp.concatenate([near, jnp.full_like(near[:1], -1.0)], axis=0), "lower",
    )
    last = best_of(
        [[(0, "all"), (1, "all")]] * 3 + [[(0, "all"), (1, "all"), (2, "all"), (3, "all")]],
        [deep, deep_twin, below, below_twin], [mine, side, above, far], flags,
        jnp.concatenate([lower, jnp.full_like(near[:1], -1.0)], axis=0), "last",
    )
    lift = [(t, s) for s, t in fall]
    tilt = [(t, s) for s, t in slant]
    from_side = sent(last[1], across)
    from_below = sent(last[2], lift)
    from_slant = sent(last[3], tilt)
    top = layer == LAYERS - 1
    outer = jnp.where(top, jnp.maximum(from_below, from_slant), -1.0)
    return jnp.maximum(jnp.maximum(last[0], from_side), outer)


def per_device(embeddings, cluster_id):
    if lax.axis_size("wide") == 4 * LAYERS:
        return layered(embeddings, cluster_id)
    return routed(embeddings, cluster_id)


def solution(mesh):
    placed = (P(("dom", "wide"), None), P(("dom", "wide"), None))
    return jax.shard_map(
        per_device, mesh=mesh, in_specs=placed, out_specs=P(("dom", "wide")), check_vma=False
    )
```

```python
import functools
import math

import jax
import jax.numpy as jnp
from jax import lax
from jax.experimental import pallas as pl
from jax.experimental.pallas import tpu as pltpu
from jax.sharding import PartitionSpec as P


def swapped(value, axis, bit):
    mask = 2**bit
    pairs = [(source, source ^ mask) for source in range(lax.axis_size(axis))]
    return lax.ppermute(value, axis, pairs)


def normalize(embedded):
    values = embedded.astype(jnp.float32)
    inverse = lax.rsqrt(jnp.mean(values * values, axis=1, keepdims=True) + 1e-06)
    return (values * inverse * (1.0 / math.sqrt(values.shape[1]))).astype(jnp.bfloat16)


def pair_scores(queries, key_rows):
    return jnp.einsum("qd,kd->qk", queries, key_rows, preferred_element_type=jnp.float32)


def masked_max(scores, allowed):
    return jnp.max(jnp.where(allowed, scores, -1.0), axis=1)


def routed(embeddings, cluster_id):
    axis_size = lax.axis_size("wide")
    rows_dev = embeddings.shape[0]
    feature_dim = embeddings.shape[1]
    clusters = axis_size // 2
    capacity = (5 * rows_dev + 2 * axis_size - 1) // (2 * axis_size)
    buffer_rows = axis_size * capacity
    unit_rows = normalize(embeddings)
    labels = cluster_id[:, 0]
    my_index = lax.axis_index("wide")
    my_flip = my_index % 2
    position = lax.iota(jnp.int32, rows_dev)
    same_cluster = labels[:, None] == labels[None, :]
    earlier = position[None, :] < position[:, None]
    local_rank = jnp.sum((same_cluster & earlier).astype(jnp.int32), axis=1)
    target = 2 * labels + (local_rank + my_flip) % 2
    slot_index = target * capacity + local_rank // 2
    outgoing = jnp.zeros((buffer_rows, feature_dim), jnp.bfloat16).at[slot_index].set(unit_rows)
    cluster_count = jnp.sum(
        (labels[:, None] == lax.iota(jnp.int32, clusters)[None, :]).astype(jnp.int32), axis=0
    )
    parity = lax.iota(jnp.int32, axis_size) % 2
    send_count = (jnp.repeat(cluster_count, 2) + 1 - (parity + my_flip) % 2) // 2
    outgoing_blocks = outgoing.reshape(axis_size, capacity, feature_dim)
    count_blocks = send_count.reshape(axis_size, 1)
    received, counts = (
        lax.all_to_all(outgoing_blocks, "wide", split_axis=0, concat_axis=0, tiled=True),
        lax.all_to_all(count_blocks, "wide", split_axis=0, concat_axis=0, tiled=True),
    )
    own_rows = received.reshape(buffer_rows, feature_dim)
    partner, partner_counts = swapped((own_rows, counts), "wide", 0)
    side_bit = my_index % 2
    slot_pos = lax.iota(jnp.int32, capacity)
    sources = lax.iota(jnp.int32, axis_size)
    base_key = (sources[:, None] * (2 * capacity) + 2 * slot_pos[None, :]).reshape(-1)
    source_parity = jnp.repeat(sources % 2, capacity)
    own_key = base_key + (side_bit + source_parity) % 2
    partner_key = base_key + (1 - side_bit + source_parity) % 2
    own_live = (slot_pos[None, :] < counts).reshape(-1)
    partner_live = (slot_pos[None, :] < partner_counts).reshape(-1)
    blocks = 8
    query_rows = own_rows.reshape(blocks, -1, feature_dim)
    query_key = own_key.reshape(blocks, -1)

    def self_max(pieces):
        queries, keys_here = pieces
        return masked_max(
            pair_scores(queries, own_rows),
            own_live[None, :] & (own_key[None, :] < keys_here[:, None]),
        )

    self_best = lax.map(self_max, (query_rows, query_key)).reshape(-1)
    first = side_bit == 0
    left_rows = jnp.where(first, own_rows, partner)
    left_key = jnp.where(first, own_key, partner_key)
    left_live = jnp.where(first, own_live, partner_live)
    right_rows = jnp.where(first, partner, own_rows)
    right_key = jnp.where(first, partner_key, own_key)
    right_live = jnp.where(first, partner_live, own_live)
    half_rows = buffer_rows // 2
    start = side_bit * half_rows
    lower_rows = lax.dynamic_slice_in_dim(left_rows, start, half_rows, 0).reshape(
        blocks // 2, -1, feature_dim
    )
    lower_key = lax.dynamic_slice_in_dim(left_key, start, half_rows, 0).reshape(blocks // 2, -1)
    lower_live = lax.dynamic_slice_in_dim(left_live, start, half_rows, 0).reshape(blocks // 2, -1)

    def cross_max(pieces):
        queries, keys_here, live_here = pieces
        scores = pair_scores(queries, right_rows)
        row_best = masked_max(
            scores, right_live[None, :] & (right_key[None, :] < keys_here[:, None])
        )
        column_mask = live_here[:, None] & (keys_here[:, None] < right_key[None, :])
        column_best = jnp.max(jnp.where(column_mask, scores, -1.0), axis=0)
        return (row_best, column_best)

    row_best, column_best = lax.map(cross_max, (lower_rows, lower_key, lower_live))
    row_best = row_best.reshape(-1)
    column_best = jnp.max(column_best, axis=0)
    placed = lax.dynamic_update_slice_in_dim(
        jnp.full((buffer_rows,), -1.0, jnp.float32), row_best, start, 0
    )
    kept = jnp.where(first, placed, column_best)
    handed = jnp.where(first, column_best, placed)
    returned = swapped(handed, "wide", 0)
    best_all = jnp.maximum(self_best, jnp.maximum(kept, returned))
    back = lax.all_to_all(
        best_all.reshape(axis_size, capacity), "wide", split_axis=0, concat_axis=0, tiled=True
    )
    return back.reshape(-1)[slot_index]


LAYERS = 4
TAG_ROWS = 16
PARAMS = pltpu.CompilerParams(vmem_limit_bytes=16 * 1024 * 1024)


def tag_kernel(rows_ref, label_ref, *out_refs):
    rows, width = rows_ref.shape
    codes = (label_ref[...] + 1).astype(jnp.float32)
    whole_ref, head_ref, tail_ref = out_refs
    cut = head_ref.shape[0] - TAG_ROWS
    for part_ref, low, high in ((head_ref, 0, cut), (tail_ref, cut, rows)):
        values = rows_ref[low:high, :].astype(jnp.float32)
        inverse = lax.rsqrt(jnp.mean(values * values, axis=1, keepdims=True) + 1e-06)
        unit = (values * inverse * (1.0 / math.sqrt(width))).astype(jnp.bfloat16)
        whole_ref[low:high, :] = unit
        part_ref[: high - low, :] = unit
    for ref, low, high in ((whole_ref, 0, rows), (head_ref, 0, cut), (tail_ref, cut, rows)):
        count = high - low
        line = jnp.broadcast_to(codes[:, low:high], (TAG_ROWS, count)).astype(jnp.bfloat16)
        ref[count:, :count] = line
        if count < width:
            ref[count:, count:] = jnp.zeros((TAG_ROWS, width - count), jnp.bfloat16)


def tagged(embeddings, labels, cut):
    rows, width = embeddings.shape
    counts = (rows, cut, rows - cut)
    return pl.pallas_call(
        tag_kernel,
        out_shape=[pltpu.VMEM((count + TAG_ROWS, width), jnp.bfloat16) for count in counts],
        compiler_params=PARAMS,
        name="tagged",
    )(embeddings, labels.reshape(1, rows))


def code_row(block_ref):
    rows = block_ref.shape[0] - TAG_ROWS
    return block_ref[rows:, :rows].astype(jnp.float32)[:1]


def best_kernel(tasks, n_keys, n_queries, n_begun, *refs):
    key_refs = refs[:n_keys]
    query_refs = refs[n_keys : n_keys + n_queries]
    begun_refs = refs[n_keys + n_queries : n_keys + n_queries + n_begun]
    out_refs = refs[n_keys + n_queries + n_begun :]
    index = lax.axis_index("wide")
    switches = {"core": index % 2 == 1, "column": (index // 2) % 2 == 0}
    key_codes = []
    for ref in key_refs:
        count = ref.shape[0] - TAG_ROWS
        key_codes.append(jnp.transpose(jnp.broadcast_to(code_row(ref), (128, count))))
    for q, query_ref in enumerate(query_refs):
        rows = query_ref.shape[0] - TAG_ROWS
        queries = query_ref[:rows, :]
        row_code = code_row(query_ref)
        best = [None] * (rows // 128)
        for k, mode in tasks[q]:
            code = row_code
            if mode in switches:
                code = jnp.where(switches[mode], row_code, -1.0)
            count = key_refs[k].shape[0] - TAG_ROWS
            scores = lax.dot_general(
                key_refs[k][:count, :],
                queries,
                (((1,), (1,)), ((), ())),
                preferred_element_type=jnp.float32,
            )
            for b in range(rows // 128):
                low = b * 128
                allowed = key_codes[k] == code[:, low : low + 128]
                if mode == "before":
                    key_at = lax.broadcasted_iota(jnp.int32, (count, 128), 0)
                    query_at = lax.broadcasted_iota(jnp.int32, (count, 128), 1) + low
                    allowed = allowed & (key_at < query_at)
                kept = jnp.where(allowed, scores[:, low : low + 128], -1.0)
                part = jnp.max(kept.reshape(count // 8, 8, 128), axis=0)
                best[b] = part if best[b] is None else jnp.maximum(best[b], part)
        for b, part in enumerate(best):
            low = b * 128
            line = jnp.max(part, axis=0, keepdims=True)
            if q < n_begun:
                line = jnp.maximum(line, begun_refs[q][:, low : low + 128])
            out_refs[q][:, low : low + 128] = line


def best_of(tasks, keys, queries, begun):
    arrays = [
        pltpu.with_memory_space_constraint(value, pltpu.VMEM)
        for value in list(keys) + list(queries) + list(begun)
    ]
    key_rows = [value.shape[0] - TAG_ROWS for value in keys]
    width = queries[0].shape[1]
    pairs = sum(
        key_rows[k] * (query.shape[0] - TAG_ROWS)
        for query, listed in zip(queries, tasks)
        for k, _ in listed
    )
    return pl.pallas_call(
        functools.partial(best_kernel, tasks, len(keys), len(queries), len(begun)),
        out_shape=[pltpu.VMEM((1, value.shape[0] - TAG_ROWS), jnp.float32) for value in queries],
        in_specs=[pl.BlockSpec(memory_space=pltpu.VMEM)] * len(arrays),
        cost_estimate=pl.CostEstimate(
            flops=2 * pairs * width,
            transcendentals=0,
            bytes_accessed=sum(value.nbytes for value in arrays),
        ),
        compiler_params=PARAMS,
    )(*arrays)


def every(keys):
    return [(k, "all") for k in keys]


def layered(embeddings, cluster_id):
    rows = embeddings.shape[0]
    mine, head, tail = tagged(embeddings, cluster_id[:, 0], rows * 3 // 4)
    spots = [(z, x, c) for z in range(LAYERS) for x in range(2) for c in range(2)]

    def at(z, x, c):
        return (z * 2 + x) * 2 + c

    def sent(value, hops):
        return lax.ppermute(value, "wide", hops)

    across = [(at(z, x, c), at(z, 1 - x, c)) for z, x, c in spots]
    beside = [(at(z, x, c), at(z, x, 1 - c)) for z, x, c in spots]
    rise = [(at(z, x, c), at(z + 1, x, c)) for z, x, c in spots if z + 1 < LAYERS]
    relay = [(at(z, x, c), at(z + 1, x, c)) for z, x, c in spots if z == 1]
    fall = [(at(z, x, c), at(z - 1, x, c)) for z, x, c in spots if z == LAYERS - 1]
    slant = [(at(z, x, c), at(z - 1, 1 - x, c)) for z, x, c in spots if z == LAYERS - 1]

    below_head = sent(head, rise)
    above = sent(mine, fall)
    side = sent(mine, across)
    below_tail = sent(tail, rise)
    twin = sent(mine, beside)
    far = sent(mine, slant)
    below = [
        below_head, sent(below_head, beside),
        below_tail, sent(below_tail, beside),
    ]
    deep_head = sent(below_head, relay)
    deep_tail = sent(below_tail, relay)
    deep_first = [deep_head, sent(deep_head, beside)]
    deep_last = [deep_tail, sent(deep_tail, beside)]

    own = best_of([[(0, "before"), (1, "core")]], [mine, twin], [mine], [])
    here = best_of(
        [every([2, 3, 4, 5]), [(0, "column"), (1, "column")] + every([2, 3, 4, 5]), every([2, 3, 4, 5])],
        [mine, twin] + below, [mine, side, above], own,
    )
    deeper = best_of([every([0, 1])] * 3, deep_first, [mine, side, above], here)
    last = best_of(
        [every([0, 1])] * 3 + [every(range(8))],
        deep_last + deep_first + below, [mine, side, above, far], deeper,
    )
    lift = [(t, s) for s, t in fall]
    tilt = [(t, s) for s, t in slant]
    from_slant = sent(last[3], tilt)
    from_side = sent(last[1], across)
    from_below = sent(last[2], lift)
    top = lax.axis_index("wide") // 4 == LAYERS - 1
    outer = jnp.where(top, jnp.maximum(from_below, from_slant), -1.0)
    return jnp.maximum(jnp.maximum(last[0], from_side), outer)[0]


def per_device(embeddings, cluster_id):
    if lax.axis_size("wide") == 4 * LAYERS:
        return layered(embeddings, cluster_id)
    return routed(embeddings, cluster_id)


def solution(mesh):
    placed = (P(("dom", "wide"), None), P(("dom", "wide"), None))
    return jax.shard_map(
        per_device, mesh=mesh, in_specs=placed, out_specs=P(("dom", "wide")), check_vma=False
    )
```

```python
import functools
import math

import jax
import jax.numpy as jnp
from jax import lax
from jax.experimental import pallas as pl
from jax.experimental.pallas import tpu as pltpu
from jax.sharding import PartitionSpec as P


def swapped(value, axis, bit):
    mask = 2**bit
    pairs = [(source, source ^ mask) for source in range(lax.axis_size(axis))]
    return lax.ppermute(value, axis, pairs)


def normalize(embedded):
    values = embedded.astype(jnp.float32)
    inverse = lax.rsqrt(jnp.mean(values * values, axis=1, keepdims=True) + 1e-06)
    return (values * inverse * (1.0 / math.sqrt(values.shape[1]))).astype(jnp.bfloat16)


def pair_scores(queries, key_rows):
    return jnp.einsum("qd,kd->qk", queries, key_rows, preferred_element_type=jnp.float32)


def masked_max(scores, allowed):
    return jnp.max(jnp.where(allowed, scores, -1.0), axis=1)


def routed(embeddings, cluster_id):
    axis_size = lax.axis_size("wide")
    rows_dev = embeddings.shape[0]
    feature_dim = embeddings.shape[1]
    clusters = axis_size // 2
    capacity = (5 * rows_dev + 2 * axis_size - 1) // (2 * axis_size)
    buffer_rows = axis_size * capacity
    unit_rows = normalize(embeddings)
    labels = cluster_id[:, 0]
    my_index = lax.axis_index("wide")
    my_flip = my_index % 2
    position = lax.iota(jnp.int32, rows_dev)
    same_cluster = labels[:, None] == labels[None, :]
    earlier = position[None, :] < position[:, None]
    local_rank = jnp.sum((same_cluster & earlier).astype(jnp.int32), axis=1)
    target = 2 * labels + (local_rank + my_flip) % 2
    slot_index = target * capacity + local_rank // 2
    outgoing = jnp.zeros((buffer_rows, feature_dim), jnp.bfloat16).at[slot_index].set(unit_rows)
    cluster_count = jnp.sum(
        (labels[:, None] == lax.iota(jnp.int32, clusters)[None, :]).astype(jnp.int32), axis=0
    )
    parity = lax.iota(jnp.int32, axis_size) % 2
    send_count = (jnp.repeat(cluster_count, 2) + 1 - (parity + my_flip) % 2) // 2
    outgoing_blocks = outgoing.reshape(axis_size, capacity, feature_dim)
    count_blocks = send_count.reshape(axis_size, 1)
    received, counts = (
        lax.all_to_all(outgoing_blocks, "wide", split_axis=0, concat_axis=0, tiled=True),
        lax.all_to_all(count_blocks, "wide", split_axis=0, concat_axis=0, tiled=True),
    )
    own_rows = received.reshape(buffer_rows, feature_dim)
    partner, partner_counts = swapped((own_rows, counts), "wide", 0)
    side_bit = my_index % 2
    slot_pos = lax.iota(jnp.int32, capacity)
    sources = lax.iota(jnp.int32, axis_size)
    base_key = (sources[:, None] * (2 * capacity) + 2 * slot_pos[None, :]).reshape(-1)
    source_parity = jnp.repeat(sources % 2, capacity)
    own_key = base_key + (side_bit + source_parity) % 2
    partner_key = base_key + (1 - side_bit + source_parity) % 2
    own_live = (slot_pos[None, :] < counts).reshape(-1)
    partner_live = (slot_pos[None, :] < partner_counts).reshape(-1)
    blocks = 8
    query_rows = own_rows.reshape(blocks, -1, feature_dim)
    query_key = own_key.reshape(blocks, -1)

    def self_max(pieces):
        queries, keys_here = pieces
        return masked_max(
            pair_scores(queries, own_rows),
            own_live[None, :] & (own_key[None, :] < keys_here[:, None]),
        )

    self_best = lax.map(self_max, (query_rows, query_key)).reshape(-1)
    first = side_bit == 0
    left_rows = jnp.where(first, own_rows, partner)
    left_key = jnp.where(first, own_key, partner_key)
    left_live = jnp.where(first, own_live, partner_live)
    right_rows = jnp.where(first, partner, own_rows)
    right_key = jnp.where(first, partner_key, own_key)
    right_live = jnp.where(first, partner_live, own_live)
    half_rows = buffer_rows // 2
    start = side_bit * half_rows
    lower_rows = lax.dynamic_slice_in_dim(left_rows, start, half_rows, 0).reshape(
        blocks // 2, -1, feature_dim
    )
    lower_key = lax.dynamic_slice_in_dim(left_key, start, half_rows, 0).reshape(blocks // 2, -1)
    lower_live = lax.dynamic_slice_in_dim(left_live, start, half_rows, 0).reshape(blocks // 2, -1)

    def cross_max(pieces):
        queries, keys_here, live_here = pieces
        scores = pair_scores(queries, right_rows)
        row_best = masked_max(
            scores, right_live[None, :] & (right_key[None, :] < keys_here[:, None])
        )
        column_mask = live_here[:, None] & (keys_here[:, None] < right_key[None, :])
        column_best = jnp.max(jnp.where(column_mask, scores, -1.0), axis=0)
        return (row_best, column_best)

    row_best, column_best = lax.map(cross_max, (lower_rows, lower_key, lower_live))
    row_best = row_best.reshape(-1)
    column_best = jnp.max(column_best, axis=0)
    placed = lax.dynamic_update_slice_in_dim(
        jnp.full((buffer_rows,), -1.0, jnp.float32), row_best, start, 0
    )
    kept = jnp.where(first, placed, column_best)
    handed = jnp.where(first, column_best, placed)
    returned = swapped(handed, "wide", 0)
    best_all = jnp.maximum(self_best, jnp.maximum(kept, returned))
    back = lax.all_to_all(
        best_all.reshape(axis_size, capacity), "wide", split_axis=0, concat_axis=0, tiled=True
    )
    return back.reshape(-1)[slot_index]


LAYERS = 4
TAG_ROWS = 8
LANES = 128
PARAMS = pltpu.CompilerParams(vmem_limit_bytes=16 * 1024 * 1024)


def tag_kernel(rows_hbm, label_hbm, whole_ref, head_ref, tail_ref, rows_ref, label_ref, done):
    rows, width = rows_ref.shape
    cut = head_ref.shape[0] - TAG_ROWS
    spans = [(low, low + rows // 4) for low in range(0, rows, rows // 4)]
    labels = pltpu.make_async_copy(label_hbm, label_ref, done.at[len(spans)])
    labels.start()
    copies = []
    for at, (low, high) in enumerate(spans):
        part = pl.ds(low, high - low)
        copies.append(pltpu.make_async_copy(rows_hbm.at[part], rows_ref.at[part], done.at[at]))
        copies[-1].start()
    labels.wait()
    codes = (label_ref[...] + 1).astype(jnp.float32)
    line = jnp.broadcast_to(codes, (TAG_ROWS, rows)).astype(jnp.bfloat16)
    for ref, count in ((whole_ref, rows), (head_ref, cut)):
        ref[count:, :rows] = line
        if rows < width:
            ref[count:, rows:] = jnp.zeros((TAG_ROWS, width - rows), jnp.bfloat16)
    for copy, (low, high) in zip(copies, spans):
        copy.wait()
        values = rows_ref[low:high, :].astype(jnp.float32)
        inverse = lax.rsqrt(jnp.mean(values * values, axis=1, keepdims=True) + 1e-06)
        unit = (values * inverse * (1.0 / math.sqrt(width))).astype(jnp.bfloat16)
        whole_ref[low:high, :] = unit
        if high <= cut:
            head_ref[low:high, :] = unit
        else:
            tail_ref[low - cut : high - cut, :] = unit


def tagged(embeddings, labels):
    rows, width = embeddings.shape
    labels = labels.reshape(1, rows)
    cut = rows * 3 // 4
    shapes = ((rows + TAG_ROWS, width), (cut + TAG_ROWS, width), (rows - cut, width))
    return pl.pallas_call(
        tag_kernel,
        out_shape=[pltpu.VMEM(shape, jnp.bfloat16) for shape in shapes],
        in_specs=[pl.BlockSpec(memory_space=pltpu.HBM)] * 2,
        scratch_shapes=[
            pltpu.VMEM((rows, width), jnp.bfloat16),
            pltpu.VMEM((1, rows), jnp.int32),
            pltpu.SemaphoreType.DMA((5,)),
        ],
        compiler_params=PARAMS,
        name="tagged",
    )(*[pltpu.with_memory_space_constraint(value, pltpu.HBM) for value in (embeddings, labels)])


class Block:
    def __init__(self, rows_ref, tag_ref, low, count):
        self.rows_ref = rows_ref
        self.tag_ref = tag_ref
        self.low = low
        self.count = count

    def rows(self):
        return self.rows_ref[: self.count, :]

    def codes(self):
        tags = self.tag_ref[self.tag_ref.shape[0] - TAG_ROWS :, self.low : self.low + self.count]
        return tags.astype(jnp.float32)[:1]

    def columns(self):
        return jnp.transpose(jnp.broadcast_to(self.codes(), (LANES, self.count)))


def whole(ref):
    return [Block(ref, ref, 0, ref.shape[0] - TAG_ROWS)]


def split(head_ref, tail_ref):
    cut = head_ref.shape[0] - TAG_ROWS
    return [
        Block(head_ref, head_ref, 0, cut),
        Block(tail_ref, head_ref, cut, tail_ref.shape[0]),
    ]


def halves(upper_ref, lower_ref):
    count = upper_ref.shape[0]
    return [Block(upper_ref, lower_ref, 0, count), Block(lower_ref, lower_ref, count, count)]


def raise_best(out_ref, low, query, keys, switch=None, before=False):
    codes = query.codes()
    if switch is not None:
        codes = jnp.where(switch, codes, -1.0)
    queries = query.rows()
    best = [None] * (query.count // LANES)
    merged = len(keys) > 1 and all(key.count < 2 * LANES for key in keys)
    pieces = [keys] if merged else [[key] for key in keys]
    for piece in pieces:
        rows = jnp.concatenate([key.rows() for key in piece], axis=0) if merged else piece[0].rows()
        columns = [key.columns() for key in piece]
        columns = jnp.concatenate(columns, axis=0) if merged else columns[0]
        count = rows.shape[0]
        scores = lax.dot_general(
            rows, queries, (((1,), (1,)), ((), ())), preferred_element_type=jnp.float32
        )
        for b in range(query.count // LANES):
            span = slice(b * LANES, (b + 1) * LANES)
            allowed = columns == codes[:, span]
            if before:
                key_at = lax.broadcasted_iota(jnp.int32, (count, LANES), 0)
                query_at = lax.broadcasted_iota(jnp.int32, (count, LANES), 1) + b * LANES
                allowed = allowed & (key_at < query_at)
            kept = jnp.where(allowed, scores[:, span], -1.0)
            part = jnp.max(kept.reshape(count // 8, 8, LANES), axis=0)
            best[b] = part if best[b] is None else jnp.maximum(best[b], part)
    for b, part in enumerate(best):
        span = slice(low + b * LANES, low + (b + 1) * LANES)
        line = jnp.max(part, axis=0, keepdims=True)
        out_ref[:, span] = jnp.maximum(out_ref[:, span], line)


def raise_all(outs, queries, keys):
    for out_ref, blocks in zip(outs, queries):
        for block in blocks:
            raise_best(out_ref, block.low, block, keys)


def place():
    index = lax.axis_index("wide")
    return index // 4, (index // 2) % 2, index % 2


def own_kernel(mine_ref, twin_ref, out_ref):
    core = place()[2]
    out_ref[...] = jnp.full(out_ref.shape, -1.0, jnp.float32)
    mine = whole(mine_ref)[0]
    raise_best(out_ref, 0, mine, whole(mine_ref), before=True)

    @pl.when(core == 1)
    def _():
        raise_best(out_ref, 0, mine, whole(twin_ref))


def here_kernel(
    own_ref, mine_ref, twin_ref, side_ref, ridge_ref, ridge_twin_ref,
    head_ref, head_twin_ref, tail_ref, tail_twin_ref, mine_out, side_out, above_out,
):
    layer, column, _ = place()
    mine_out[...] = own_ref[...]
    for ref in (side_out, above_out):
        ref[...] = jnp.full(ref.shape, -1.0, jnp.float32)
    near = [whole(mine_ref), whole(side_ref)]

    @pl.when(column == 0)
    def _():
        raise_all([side_out], [whole(side_ref)], whole(mine_ref) + whole(twin_ref))

    @pl.when(layer % 2 == 1)
    def _():
        keys = split(head_ref, tail_ref) + split(head_twin_ref, tail_twin_ref)
        raise_all([mine_out, side_out], near, keys)

    @pl.when(layer == 2)
    def _():
        keys = whole(ridge_ref) + whole(ridge_twin_ref)
        above = split(head_ref, tail_ref)
        raise_all([mine_out, side_out, above_out], near + [above], keys)


VIEWS = {
    "whole": whole,
    "split": split,
    "halves": halves,
    "end": lambda head_ref, tail_ref: split(head_ref, tail_ref)[1:],
}


def seen(views, refs):
    listed = []
    for view, count in views:
        listed.append(VIEWS[view](*refs[:count]))
        refs = refs[count:]
    return listed, refs


def deep_kernel(queries, keys, started, *refs):
    layer = place()[0]
    begun, refs = (refs[: len(queries)], refs[len(queries) :]) if started else ((), refs)
    query_blocks, refs = seen(queries, refs)
    key_blocks, outs = seen(keys, refs)
    for at, ref in enumerate(outs):
        ref[...] = begun[at][...] if started else jnp.full(ref.shape, -1.0, jnp.float32)

    @pl.when(layer == 2)
    def _():
        raise_all(outs, query_blocks, [block for blocks in key_blocks for block in blocks])


def scored(body, outputs, pairs, *arrays):
    width = arrays[-1].shape[1]
    return pl.pallas_call(
        body,
        out_shape=[pltpu.VMEM((1, count), jnp.float32) for count in outputs],
        in_specs=[pl.BlockSpec(memory_space=pltpu.VMEM)] * len(arrays),
        cost_estimate=pl.CostEstimate(
            flops=2 * pairs * width,
            transcendentals=0,
            bytes_accessed=sum(value.nbytes for value in arrays),
        ),
        compiler_params=PARAMS,
    )(*[pltpu.with_memory_space_constraint(value, pltpu.VMEM) for value in arrays])


def deepened(begun, queries, keys):
    def views(blocks):
        return tuple((view, len(arrays)) for view, *arrays in blocks)

    rows = [sum(value.shape[0] for value in arrays) // LANES * LANES for _, *arrays in queries]
    ends = [arrays[-1].shape[0] // LANES * LANES for _, *arrays in keys]
    started = begun is not None
    body = functools.partial(deep_kernel, views(queries), views(keys), started)
    arrays = [value for _, *values in (*queries, *keys) for value in values]
    pairs = sum(rows) * sum(ends)
    return scored(body, rows, pairs, *(begun if started else ()), *arrays)


def layered(embeddings, cluster_id):
    rows = embeddings.shape[0]
    mine, head, tail = tagged(embeddings, cluster_id[:, 0])
    spots = [(z, x, c) for z in range(LAYERS) for x in range(2) for c in range(2)]

    def hops(move):
        def at(z, x, c):
            return (z * 2 + x) * 2 + c

        return [(at(*spot), at(*move(*spot))) for spot in spots]

    across = hops(lambda z, x, c: (z, 1 - x, c))
    beside = hops(lambda z, x, c: (z, x, 1 - c))
    outer = hops(lambda z, x, c: (z ^ 1, x, c))
    inner = hops(lambda z, x, c: (z, x, 1 - c) if z in (0, 3) else (3 - z, x, c))
    lift = [hop for hop in outer if hop[0] // 4 == 2]
    tilt = [(source, target ^ 2) for source, target in lift]

    def sent(value, pairs):
        return lax.ppermute(value, "wide", pairs)

    near_head = sent(head, outer)
    ridge = sent(mine, inner)
    side = sent(mine, across)
    near_tail = sent(tail, outer)
    twin = sent(mine, beside)
    deep_head = sent(near_head, inner)
    upper = sent(near_head[: rows // 2], across)
    lower = sent(side[rows // 2 :], outer)
    near_head_twin = sent(near_head, beside)
    deep_tail = sent(near_tail, inner)
    near_tail_twin = sent(near_tail, beside)
    ridge_twin = sent(ridge, beside)
    deep_head_twin = sent(deep_head, beside)
    deep_tail_twin = sent(deep_tail, beside)

    square = rows * rows
    (own,) = scored(own_kernel, [rows], 2 * square, mine, twin)
    first, second, third = scored(
        here_kernel, [rows] * 3, 8 * square,
        own, mine, twin, side, ridge, ridge_twin, near_head, near_head_twin, near_tail, near_tail_twin,
    )
    flat = [("whole", mine), ("whole", side)]
    steep = [("split", near_head, near_tail), ("halves", upper, lower)]
    (fourth,) = deepened(None, steep[1:], [("whole", ridge), ("whole", ridge_twin)])
    best = deepened([first, second, third, fourth], flat + steep, [("whole", deep_head)])
    other = [("whole", deep_head_twin)]
    best_steep = deepened(best[2:], steep, other)
    best_flat = deepened(best[:2], flat, other)
    ends = [("end", deep_head, deep_tail), ("end", deep_head_twin, deep_tail_twin)]
    third, fourth = deepened(best_steep, steep, ends)
    first, second = deepened(best_flat, flat, ends)
    from_below = sent(third, lift)
    from_slant = sent(fourth, tilt)
    from_side = sent(second, across)
    top = lax.axis_index("wide") // 4 == LAYERS - 1
    under = jnp.where(top, jnp.maximum(from_below, from_slant), -1.0)
    return jnp.maximum(jnp.maximum(first, from_side), under)[0]


def per_device(embeddings, cluster_id):
    if lax.axis_size("wide") == 4 * LAYERS:
        return layered(embeddings, cluster_id)
    return routed(embeddings, cluster_id)


def solution(mesh):
    placed = (P(("dom", "wide"), None), P(("dom", "wide"), None))
    return jax.shard_map(
        per_device, mesh=mesh, in_specs=placed, out_specs=P(("dom", "wide")), check_vma=False
    )
```

```python
import functools
import math

import jax
import jax.numpy as jnp
from jax import lax
from jax.experimental import pallas as pl
from jax.experimental.pallas import tpu as pltpu
from jax.sharding import PartitionSpec as P


def swapped(value, axis, bit):
    mask = 2**bit
    pairs = [(source, source ^ mask) for source in range(lax.axis_size(axis))]
    return lax.ppermute(value, axis, pairs)


def normalize(embedded):
    values = embedded.astype(jnp.float32)
    inverse = lax.rsqrt(jnp.mean(values * values, axis=1, keepdims=True) + 1e-06)
    return (values * inverse * (1.0 / math.sqrt(values.shape[1]))).astype(jnp.bfloat16)


def pair_scores(queries, key_rows):
    return jnp.einsum("qd,kd->qk", queries, key_rows, preferred_element_type=jnp.float32)


def masked_max(scores, allowed):
    return jnp.max(jnp.where(allowed, scores, -1.0), axis=1)


def routed(embeddings, cluster_id):
    axis_size = lax.axis_size("wide")
    rows_dev = embeddings.shape[0]
    feature_dim = embeddings.shape[1]
    clusters = axis_size // 2
    capacity = (5 * rows_dev + 2 * axis_size - 1) // (2 * axis_size)
    buffer_rows = axis_size * capacity
    unit_rows = normalize(embeddings)
    labels = cluster_id[:, 0]
    my_index = lax.axis_index("wide")
    my_flip = my_index % 2
    position = lax.iota(jnp.int32, rows_dev)
    same_cluster = labels[:, None] == labels[None, :]
    earlier = position[None, :] < position[:, None]
    local_rank = jnp.sum((same_cluster & earlier).astype(jnp.int32), axis=1)
    target = 2 * labels + (local_rank + my_flip) % 2
    slot_index = target * capacity + local_rank // 2
    outgoing = jnp.zeros((buffer_rows, feature_dim), jnp.bfloat16).at[slot_index].set(unit_rows)
    cluster_count = jnp.sum(
        (labels[:, None] == lax.iota(jnp.int32, clusters)[None, :]).astype(jnp.int32), axis=0
    )
    parity = lax.iota(jnp.int32, axis_size) % 2
    send_count = (jnp.repeat(cluster_count, 2) + 1 - (parity + my_flip) % 2) // 2
    outgoing_blocks = outgoing.reshape(axis_size, capacity, feature_dim)
    count_blocks = send_count.reshape(axis_size, 1)
    received, counts = (
        lax.all_to_all(outgoing_blocks, "wide", split_axis=0, concat_axis=0, tiled=True),
        lax.all_to_all(count_blocks, "wide", split_axis=0, concat_axis=0, tiled=True),
    )
    own_rows = received.reshape(buffer_rows, feature_dim)
    partner, partner_counts = swapped((own_rows, counts), "wide", 0)
    side_bit = my_index % 2
    slot_pos = lax.iota(jnp.int32, capacity)
    sources = lax.iota(jnp.int32, axis_size)
    base_key = (sources[:, None] * (2 * capacity) + 2 * slot_pos[None, :]).reshape(-1)
    source_parity = jnp.repeat(sources % 2, capacity)
    own_key = base_key + (side_bit + source_parity) % 2
    partner_key = base_key + (1 - side_bit + source_parity) % 2
    own_live = (slot_pos[None, :] < counts).reshape(-1)
    partner_live = (slot_pos[None, :] < partner_counts).reshape(-1)
    blocks = 8
    query_rows = own_rows.reshape(blocks, -1, feature_dim)
    query_key = own_key.reshape(blocks, -1)

    def self_max(pieces):
        queries, keys_here = pieces
        return masked_max(
            pair_scores(queries, own_rows),
            own_live[None, :] & (own_key[None, :] < keys_here[:, None]),
        )

    self_best = lax.map(self_max, (query_rows, query_key)).reshape(-1)
    first = side_bit == 0
    left_rows = jnp.where(first, own_rows, partner)
    left_key = jnp.where(first, own_key, partner_key)
    left_live = jnp.where(first, own_live, partner_live)
    right_rows = jnp.where(first, partner, own_rows)
    right_key = jnp.where(first, partner_key, own_key)
    right_live = jnp.where(first, partner_live, own_live)
    half_rows = buffer_rows // 2
    start = side_bit * half_rows
    lower_rows = lax.dynamic_slice_in_dim(left_rows, start, half_rows, 0).reshape(
        blocks // 2, -1, feature_dim
    )
    lower_key = lax.dynamic_slice_in_dim(left_key, start, half_rows, 0).reshape(blocks // 2, -1)
    lower_live = lax.dynamic_slice_in_dim(left_live, start, half_rows, 0).reshape(blocks // 2, -1)

    def cross_max(pieces):
        queries, keys_here, live_here = pieces
        scores = pair_scores(queries, right_rows)
        row_best = masked_max(
            scores, right_live[None, :] & (right_key[None, :] < keys_here[:, None])
        )
        column_mask = live_here[:, None] & (keys_here[:, None] < right_key[None, :])
        column_best = jnp.max(jnp.where(column_mask, scores, -1.0), axis=0)
        return (row_best, column_best)

    row_best, column_best = lax.map(cross_max, (lower_rows, lower_key, lower_live))
    row_best = row_best.reshape(-1)
    column_best = jnp.max(column_best, axis=0)
    placed = lax.dynamic_update_slice_in_dim(
        jnp.full((buffer_rows,), -1.0, jnp.float32), row_best, start, 0
    )
    kept = jnp.where(first, placed, column_best)
    handed = jnp.where(first, column_best, placed)
    returned = swapped(handed, "wide", 0)
    best_all = jnp.maximum(self_best, jnp.maximum(kept, returned))
    back = lax.all_to_all(
        best_all.reshape(axis_size, capacity), "wide", split_axis=0, concat_axis=0, tiled=True
    )
    return back.reshape(-1)[slot_index]


LAYERS = 4
TAG_ROWS = 8
LANES = 128
PARAMS = pltpu.CompilerParams(vmem_limit_bytes=16 * 1024 * 1024)


def unit_of(rows):
    values = rows.astype(jnp.float32)
    inverse = lax.rsqrt(jnp.mean(values * values, axis=1, keepdims=True) + 1e-06)
    return (values * inverse * (1.0 / math.sqrt(rows.shape[1]))).astype(jnp.bfloat16)


def tag_kernel(
    rows_hbm, label_hbm, whole_ref, head_ref, tail_ref, mark_ref, rows_ref, label_ref, done
):
    rows, width = rows_ref.shape
    cut = head_ref.shape[0] - TAG_ROWS
    spans = [(low, low + rows // 4) for low in range(0, rows, rows // 4)]
    labels = pltpu.make_async_copy(label_hbm, label_ref, done.at[len(spans)])
    labels.start()
    copies = []
    for at, (low, high) in enumerate(spans):
        part = pl.ds(low, high - low)
        copies.append(pltpu.make_async_copy(rows_hbm.at[part], rows_ref.at[part], done.at[at]))
        copies[-1].start()
    labels.wait()
    codes = (label_ref[...] + 1).astype(jnp.float32)
    line = jnp.broadcast_to(codes, (TAG_ROWS, rows)).astype(jnp.bfloat16)
    mark_ref[...] = line
    for ref, count in ((whole_ref, rows), (head_ref, cut)):
        ref[count:, :rows] = line
        if rows < width:
            ref[count:, rows:] = jnp.zeros((TAG_ROWS, width - rows), jnp.bfloat16)
    for copy, (low, high) in zip(copies, spans):
        copy.wait()
        unit = unit_of(rows_ref[low:high, :])
        whole_ref[low:high, :] = unit
        if high <= cut:
            head_ref[low:high, :] = unit
        else:
            tail_ref[low - cut : high - cut, :] = unit


def tagged(embeddings, labels):
    rows, width = embeddings.shape
    labels = labels.reshape(1, rows)
    cut = rows // 2
    shapes = ((rows + TAG_ROWS, width), (cut + TAG_ROWS, width), (rows - cut, width), (TAG_ROWS, rows))
    return pl.pallas_call(
        tag_kernel,
        out_shape=[pltpu.VMEM(shape, jnp.bfloat16) for shape in shapes],
        in_specs=[pl.BlockSpec(memory_space=pltpu.HBM)] * 2,
        scratch_shapes=[
            pltpu.VMEM((rows, width), jnp.bfloat16),
            pltpu.VMEM((1, rows), jnp.int32),
            pltpu.SemaphoreType.DMA((5,)),
        ],
        compiler_params=PARAMS,
        name="tagged",
    )(*[pltpu.with_memory_space_constraint(value, pltpu.HBM) for value in (embeddings, labels)])


def ridge_kernel(rows_ref, mark_ref, out_ref):
    rows, width = rows_ref.shape
    out_ref[:rows, :] = unit_of(rows_ref[...])
    out_ref[rows:, :rows] = mark_ref[...]
    if rows < width:
        out_ref[rows:, rows:] = jnp.zeros((TAG_ROWS, width - rows), jnp.bfloat16)


def arrived(rows, marks):
    count, width = rows.shape
    return pl.pallas_call(
        ridge_kernel,
        out_shape=pltpu.VMEM((count + TAG_ROWS, width), jnp.bfloat16),
        in_specs=[pl.BlockSpec(memory_space=pltpu.VMEM)] * 2,
        compiler_params=PARAMS,
        name="arrived",
    )(*[pltpu.with_memory_space_constraint(value, pltpu.VMEM) for value in (rows, marks)])


class Block:
    def __init__(self, rows_ref, tag_ref, low, count):
        self.rows_ref = rows_ref
        self.tag_ref = tag_ref
        self.low = low
        self.count = count

    def rows(self):
        return self.rows_ref[: self.count, :]

    def codes(self):
        tags = self.tag_ref[self.tag_ref.shape[0] - TAG_ROWS :, self.low : self.low + self.count]
        return tags.astype(jnp.float32)[:1]

    def columns(self):
        return jnp.transpose(jnp.broadcast_to(self.codes(), (LANES, self.count)))


def whole(ref):
    return [Block(ref, ref, 0, ref.shape[0] - TAG_ROWS)]


def split(head_ref, tail_ref):
    cut = head_ref.shape[0] - TAG_ROWS
    return [
        Block(head_ref, head_ref, 0, cut),
        Block(tail_ref, head_ref, cut, tail_ref.shape[0]),
    ]


def halves(upper_ref, lower_ref):
    count = upper_ref.shape[0]
    return [Block(upper_ref, lower_ref, 0, count), Block(lower_ref, lower_ref, count, count)]


def raise_best(out_ref, low, query, keys, switch=None, before=False):
    codes = query.codes()
    if switch is not None:
        codes = jnp.where(switch, codes, -1.0)
    queries = query.rows()
    best = [None] * (query.count // LANES)
    merged = len(keys) > 1 and all(key.count < 2 * LANES for key in keys)
    pieces = [keys] if merged else [[key] for key in keys]
    for piece in pieces:
        rows = jnp.concatenate([key.rows() for key in piece], axis=0) if merged else piece[0].rows()
        columns = [key.columns() for key in piece]
        columns = jnp.concatenate(columns, axis=0) if merged else columns[0]
        count = rows.shape[0]
        scores = lax.dot_general(
            rows, queries, (((1,), (1,)), ((), ())), preferred_element_type=jnp.float32
        )
        for b in range(query.count // LANES):
            span = slice(b * LANES, (b + 1) * LANES)
            allowed = columns == codes[:, span]
            if before:
                key_at = lax.broadcasted_iota(jnp.int32, (count, LANES), 0)
                query_at = lax.broadcasted_iota(jnp.int32, (count, LANES), 1) + b * LANES
                allowed = allowed & (key_at < query_at)
            kept = jnp.where(allowed, scores[:, span], -1.0)
            part = jnp.max(kept.reshape(count // 8, 8, LANES), axis=0)
            best[b] = part if best[b] is None else jnp.maximum(best[b], part)
    for b, part in enumerate(best):
        span = slice(low + b * LANES, low + (b + 1) * LANES)
        line = jnp.max(part, axis=0, keepdims=True)
        out_ref[:, span] = jnp.maximum(out_ref[:, span], line)


def raise_all(outs, queries, keys):
    for out_ref, blocks in zip(outs, queries):
        for block in blocks:
            raise_best(out_ref, block.low, block, keys)


def place():
    index = lax.axis_index("wide")
    return index // 4, (index // 2) % 2, index % 2


def own_kernel(mine_ref, twin_ref, out_ref):
    core = place()[2]
    out_ref[...] = jnp.full(out_ref.shape, -1.0, jnp.float32)
    mine = whole(mine_ref)[0]
    raise_best(out_ref, 0, mine, whole(mine_ref), before=True)

    @pl.when(core == 1)
    def _():
        raise_best(out_ref, 0, mine, whole(twin_ref))


def here_kernel(
    own_ref, mine_ref, twin_ref, side_ref, ridge_ref, ridge_twin_ref,
    head_ref, head_twin_ref, tail_ref, tail_twin_ref, mine_out, side_out, above_out,
):
    layer, column, _ = place()
    mine_out[...] = own_ref[...]
    for ref in (side_out, above_out):
        ref[...] = jnp.full(ref.shape, -1.0, jnp.float32)
    near = [whole(mine_ref), whole(side_ref)]

    @pl.when(column == 0)
    def _():
        raise_all([side_out], [whole(side_ref)], whole(mine_ref) + whole(twin_ref))

    @pl.when(layer % 2 == 1)
    def _():
        keys = split(head_ref, tail_ref) + split(head_twin_ref, tail_twin_ref)
        raise_all([mine_out, side_out], near, keys)

    @pl.when(layer == 2)
    def _():
        keys = whole(ridge_ref) + whole(ridge_twin_ref)
        above = split(head_ref, tail_ref)
        raise_all([mine_out, side_out, above_out], near + [above], keys)


VIEWS = {
    "whole": whole,
    "split": split,
    "halves": halves,
    "end": lambda head_ref, tail_ref: split(head_ref, tail_ref)[1:],
}


def seen(views, refs):
    listed = []
    for view, count in views:
        listed.append(VIEWS[view](*refs[:count]))
        refs = refs[count:]
    return listed, refs


def deep_kernel(queries, keys, started, *refs):
    layer = place()[0]
    begun, refs = (refs[: len(queries)], refs[len(queries) :]) if started else ((), refs)
    query_blocks, refs = seen(queries, refs)
    key_blocks, outs = seen(keys, refs)
    for at, ref in enumerate(outs):
        ref[...] = begun[at][...] if started else jnp.full(ref.shape, -1.0, jnp.float32)

    @pl.when(layer == 2)
    def _():
        raise_all(outs, query_blocks, [block for blocks in key_blocks for block in blocks])


def scored(body, outputs, pairs, *arrays):
    width = arrays[-1].shape[1]
    return pl.pallas_call(
        body,
        out_shape=[pltpu.VMEM((1, count), jnp.float32) for count in outputs],
        in_specs=[pl.BlockSpec(memory_space=pltpu.VMEM)] * len(arrays),
        cost_estimate=pl.CostEstimate(
            flops=2 * pairs * width,
            transcendentals=0,
            bytes_accessed=sum(value.nbytes for value in arrays),
        ),
        compiler_params=PARAMS,
    )(*[pltpu.with_memory_space_constraint(value, pltpu.VMEM) for value in arrays])


def deepened(begun, queries, keys):
    def views(blocks):
        return tuple((view, len(arrays)) for view, *arrays in blocks)

    rows = [sum(value.shape[0] for value in arrays) // LANES * LANES for _, *arrays in queries]
    ends = [arrays[-1].shape[0] // LANES * LANES for _, *arrays in keys]
    started = begun is not None
    body = functools.partial(deep_kernel, views(queries), views(keys), started)
    arrays = [value for _, *values in (*queries, *keys) for value in values]
    pairs = sum(rows) * sum(ends)
    return scored(body, rows, pairs, *(begun if started else ()), *arrays)


def layered(embeddings, cluster_id):
    rows = embeddings.shape[0]
    spots = [(z, x, c) for z in range(LAYERS) for x in range(2) for c in range(2)]

    def hops(move):
        def at(z, x, c):
            return (z * 2 + x) * 2 + c

        return [(at(*spot), at(*move(*spot))) for spot in spots]

    across = hops(lambda z, x, c: (z, 1 - x, c))
    beside = hops(lambda z, x, c: (z, x, 1 - c))
    outer = hops(lambda z, x, c: (z ^ 1, x, c))
    inner = hops(lambda z, x, c: (z, x, 1 - c) if z in (0, 3) else (3 - z, x, c))
    lift = [hop for hop in outer if hop[0] // 4 == 2]
    tilt = [(source, target ^ 2) for source, target in lift]

    def sent(value, pairs):
        return lax.ppermute(value, "wide", pairs)

    raw_ridge = sent(embeddings, inner)
    mine, head, tail, marks = tagged(embeddings, cluster_id[:, 0])
    near_head = sent(head, outer)
    side = sent(mine, across)
    near_tail = sent(tail, outer)
    twin = sent(mine, beside)
    ridge = arrived(raw_ridge, sent(marks, inner))
    deep_head = sent(near_head, inner)
    upper = sent(near_head[: rows // 2], across)
    lower = sent(side[rows // 2 :], outer)
    near_head_twin = sent(near_head, beside)
    deep_tail = sent(near_tail, inner)
    near_tail_twin = sent(near_tail, beside)
    ridge_twin = sent(ridge, beside)
    deep_head_twin = sent(deep_head, beside)
    deep_tail_twin = sent(deep_tail, beside)

    square = rows * rows
    (own,) = scored(own_kernel, [rows], 2 * square, mine, twin)
    best = scored(
        here_kernel, [rows] * 3, 8 * square,
        own, mine, twin, side, ridge, ridge_twin, near_head, near_head_twin, near_tail, near_tail_twin,
    )
    flat = [("whole", mine), ("whole", side)]
    steep = [("split", near_head, near_tail), ("halves", upper, lower)]
    deep, deep_twin = ("whole", deep_head), ("whole", deep_head_twin)
    third, fourth = ("end", deep_head, deep_tail), ("end", deep_head_twin, deep_tail_twin)
    best = deepened(best, flat + steep[:1], [deep])
    best = deepened(best, flat + steep[:1], [deep_twin])
    keys = [("whole", ridge), ("whole", ridge_twin), deep, deep_twin]
    best_flat, best_steep = best[:2], best[2:] + deepened(None, steep[1:], keys)
    best_flat = deepened(best_flat, flat, [third])
    best_steep = deepened(best_steep, steep, [third])
    first, second = deepened(best_flat, flat, [fourth])
    third, fourth = deepened(best_steep, steep, [fourth])
    from_below = sent(third, lift)
    from_slant = sent(fourth, tilt)
    from_side = sent(second, across)
    top = lax.axis_index("wide") // 4 == LAYERS - 1
    under = jnp.where(top, jnp.maximum(from_below, from_slant), -1.0)
    return jnp.maximum(jnp.maximum(first, from_side), under)[0]


def per_device(embeddings, cluster_id):
    if lax.axis_size("wide") == 4 * LAYERS:
        return layered(embeddings, cluster_id)
    return routed(embeddings, cluster_id)


def solution(mesh):
    placed = (P(("dom", "wide"), None), P(("dom", "wide"), None))
    return jax.shard_map(
        per_device, mesh=mesh, in_specs=placed, out_specs=P(("dom", "wide")), check_vma=False
    )
```

```python
import functools
import math

import jax
import jax.numpy as jnp
from jax import lax
from jax.experimental import pallas as pl
from jax.experimental.pallas import tpu as pltpu
from jax.sharding import PartitionSpec as P


def swapped(value, axis, bit):
    mask = 2**bit
    pairs = [(source, source ^ mask) for source in range(lax.axis_size(axis))]
    return lax.ppermute(value, axis, pairs)


def normalize(embedded):
    values = embedded.astype(jnp.float32)
    inverse = lax.rsqrt(jnp.mean(values * values, axis=1, keepdims=True) + 1e-06)
    return (values * inverse * (1.0 / math.sqrt(values.shape[1]))).astype(jnp.bfloat16)


def pair_scores(queries, key_rows):
    return jnp.einsum("qd,kd->qk", queries, key_rows, preferred_element_type=jnp.float32)


def masked_max(scores, allowed):
    return jnp.max(jnp.where(allowed, scores, -1.0), axis=1)


def routed(embeddings, cluster_id):
    axis_size = lax.axis_size("wide")
    rows_dev = embeddings.shape[0]
    feature_dim = embeddings.shape[1]
    clusters = axis_size // 2
    capacity = (5 * rows_dev + 2 * axis_size - 1) // (2 * axis_size)
    buffer_rows = axis_size * capacity
    unit_rows = normalize(embeddings)
    labels = cluster_id[:, 0]
    my_index = lax.axis_index("wide")
    my_flip = my_index % 2
    position = lax.iota(jnp.int32, rows_dev)
    same_cluster = labels[:, None] == labels[None, :]
    earlier = position[None, :] < position[:, None]
    local_rank = jnp.sum((same_cluster & earlier).astype(jnp.int32), axis=1)
    target = 2 * labels + (local_rank + my_flip) % 2
    slot_index = target * capacity + local_rank // 2
    outgoing = jnp.zeros((buffer_rows, feature_dim), jnp.bfloat16).at[slot_index].set(unit_rows)
    cluster_count = jnp.sum(
        (labels[:, None] == lax.iota(jnp.int32, clusters)[None, :]).astype(jnp.int32), axis=0
    )
    parity = lax.iota(jnp.int32, axis_size) % 2
    send_count = (jnp.repeat(cluster_count, 2) + 1 - (parity + my_flip) % 2) // 2
    outgoing_blocks = outgoing.reshape(axis_size, capacity, feature_dim)
    count_blocks = send_count.reshape(axis_size, 1)
    received, counts = (
        lax.all_to_all(outgoing_blocks, "wide", split_axis=0, concat_axis=0, tiled=True),
        lax.all_to_all(count_blocks, "wide", split_axis=0, concat_axis=0, tiled=True),
    )
    own_rows = received.reshape(buffer_rows, feature_dim)
    partner, partner_counts = swapped((own_rows, counts), "wide", 0)
    side_bit = my_index % 2
    slot_pos = lax.iota(jnp.int32, capacity)
    sources = lax.iota(jnp.int32, axis_size)
    base_key = (sources[:, None] * (2 * capacity) + 2 * slot_pos[None, :]).reshape(-1)
    source_parity = jnp.repeat(sources % 2, capacity)
    own_key = base_key + (side_bit + source_parity) % 2
    partner_key = base_key + (1 - side_bit + source_parity) % 2
    own_live = (slot_pos[None, :] < counts).reshape(-1)
    partner_live = (slot_pos[None, :] < partner_counts).reshape(-1)
    blocks = 8
    query_rows = own_rows.reshape(blocks, -1, feature_dim)
    query_key = own_key.reshape(blocks, -1)

    def self_max(pieces):
        queries, keys_here = pieces
        return masked_max(
            pair_scores(queries, own_rows),
            own_live[None, :] & (own_key[None, :] < keys_here[:, None]),
        )

    self_best = lax.map(self_max, (query_rows, query_key)).reshape(-1)
    first = side_bit == 0
    left_rows = jnp.where(first, own_rows, partner)
    left_key = jnp.where(first, own_key, partner_key)
    left_live = jnp.where(first, own_live, partner_live)
    right_rows = jnp.where(first, partner, own_rows)
    right_key = jnp.where(first, partner_key, own_key)
    right_live = jnp.where(first, partner_live, own_live)
    half_rows = buffer_rows // 2
    start = side_bit * half_rows
    lower_rows = lax.dynamic_slice_in_dim(left_rows, start, half_rows, 0).reshape(
        blocks // 2, -1, feature_dim
    )
    lower_key = lax.dynamic_slice_in_dim(left_key, start, half_rows, 0).reshape(blocks // 2, -1)
    lower_live = lax.dynamic_slice_in_dim(left_live, start, half_rows, 0).reshape(blocks // 2, -1)

    def cross_max(pieces):
        queries, keys_here, live_here = pieces
        scores = pair_scores(queries, right_rows)
        row_best = masked_max(
            scores, right_live[None, :] & (right_key[None, :] < keys_here[:, None])
        )
        column_mask = live_here[:, None] & (keys_here[:, None] < right_key[None, :])
        column_best = jnp.max(jnp.where(column_mask, scores, -1.0), axis=0)
        return (row_best, column_best)

    row_best, column_best = lax.map(cross_max, (lower_rows, lower_key, lower_live))
    row_best = row_best.reshape(-1)
    column_best = jnp.max(column_best, axis=0)
    placed = lax.dynamic_update_slice_in_dim(
        jnp.full((buffer_rows,), -1.0, jnp.float32), row_best, start, 0
    )
    kept = jnp.where(first, placed, column_best)
    handed = jnp.where(first, column_best, placed)
    returned = swapped(handed, "wide", 0)
    best_all = jnp.maximum(self_best, jnp.maximum(kept, returned))
    back = lax.all_to_all(
        best_all.reshape(axis_size, capacity), "wide", split_axis=0, concat_axis=0, tiled=True
    )
    return back.reshape(-1)[slot_index]


LAYERS = 4
TAG_ROWS = 8
LANES = 128
PARAMS = pltpu.CompilerParams(vmem_limit_bytes=16 * 1024 * 1024)


def unit_of(rows):
    values = rows.astype(jnp.float32)
    inverse = lax.rsqrt(jnp.mean(values * values, axis=1, keepdims=True) + 1e-06)
    return (values * inverse * (1.0 / math.sqrt(rows.shape[1]))).astype(jnp.bfloat16)


def tag_kernel(
    rows_hbm, label_hbm, whole_ref, head_ref, tail_ref, low_ref, mark_ref, rows_ref, label_ref, done
):
    rows, width = rows_ref.shape
    cut = head_ref.shape[0] - TAG_ROWS
    spans = [(low, low + rows // 4) for low in range(0, rows, rows // 4)]
    labels = pltpu.make_async_copy(label_hbm, label_ref, done.at[len(spans)])
    labels.start()
    copies = []
    for at, (low, high) in enumerate(spans):
        part = pl.ds(low, high - low)
        copies.append(pltpu.make_async_copy(rows_hbm.at[part], rows_ref.at[part], done.at[at]))
        copies[-1].start()
    labels.wait()
    codes = (label_ref[...] + 1).astype(jnp.float32)
    line = jnp.broadcast_to(codes, (TAG_ROWS, rows)).astype(jnp.bfloat16)
    mark_ref[...] = line
    for ref, count in ((whole_ref, rows), (head_ref, cut), (low_ref, rows - cut)):
        ref[count:, :rows] = line
        if rows < width:
            ref[count:, rows:] = jnp.zeros((TAG_ROWS, width - rows), jnp.bfloat16)
    for copy, (low, high) in zip(copies, spans):
        copy.wait()
        unit = unit_of(rows_ref[low:high, :])
        whole_ref[low:high, :] = unit
        if high <= cut:
            head_ref[low:high, :] = unit
        else:
            tail_ref[low - cut : high - cut, :] = unit
            low_ref[low - cut : high - cut, :] = unit


def tagged(embeddings, labels):
    rows, width = embeddings.shape
    labels = labels.reshape(1, rows)
    cut = rows // 2
    shapes = ((rows + TAG_ROWS, width), (cut + TAG_ROWS, width), (rows - cut, width))
    shapes += ((rows - cut + TAG_ROWS, width), (TAG_ROWS, rows))
    return pl.pallas_call(
        tag_kernel,
        out_shape=[pltpu.VMEM(shape, jnp.bfloat16) for shape in shapes],
        in_specs=[pl.BlockSpec(memory_space=pltpu.HBM)] * 2,
        scratch_shapes=[
            pltpu.VMEM((rows, width), jnp.bfloat16),
            pltpu.VMEM((1, rows), jnp.int32),
            pltpu.SemaphoreType.DMA((5,)),
        ],
        compiler_params=PARAMS,
        name="tagged",
    )(*[pltpu.with_memory_space_constraint(value, pltpu.HBM) for value in (embeddings, labels)])


def ridge_kernel(rows_ref, mark_ref, out_ref):
    rows, width = rows_ref.shape
    out_ref[:rows, :] = unit_of(rows_ref[...])
    out_ref[rows:, :rows] = mark_ref[...]
    if rows < width:
        out_ref[rows:, rows:] = jnp.zeros((TAG_ROWS, width - rows), jnp.bfloat16)


def arrived(rows, marks):
    count, width = rows.shape
    return pl.pallas_call(
        ridge_kernel,
        out_shape=pltpu.VMEM((count + TAG_ROWS, width), jnp.bfloat16),
        in_specs=[pl.BlockSpec(memory_space=pltpu.VMEM)] * 2,
        compiler_params=PARAMS,
        name="arrived",
    )(*[pltpu.with_memory_space_constraint(value, pltpu.VMEM) for value in (rows, marks)])


class Block:
    def __init__(self, rows_ref, tag_ref, low, count):
        self.rows_ref = rows_ref
        self.tag_ref = tag_ref
        self.low = low
        self.count = count

    def rows(self):
        return self.rows_ref[: self.count, :]

    def codes(self):
        tags = self.tag_ref[self.tag_ref.shape[0] - TAG_ROWS :, self.low : self.low + self.count]
        return tags.astype(jnp.float32)[:1]

    def columns(self):
        return jnp.transpose(jnp.broadcast_to(self.codes(), (LANES, self.count)))


def whole(ref):
    return [Block(ref, ref, 0, ref.shape[0] - TAG_ROWS)]


def split(head_ref, tail_ref):
    cut = head_ref.shape[0] - TAG_ROWS
    return [
        Block(head_ref, head_ref, 0, cut),
        Block(tail_ref, head_ref, cut, tail_ref.shape[0]),
    ]


def paired(head_ref, low_ref):
    cut = head_ref.shape[0] - TAG_ROWS
    count = low_ref.shape[0] - TAG_ROWS
    return [Block(head_ref, head_ref, 0, cut), Block(low_ref, low_ref, cut, count)]


def halves(upper_ref, lower_ref):
    count = upper_ref.shape[0]
    return [Block(upper_ref, lower_ref, 0, count), Block(lower_ref, lower_ref, count, count)]


def raise_best(out_ref, low, query, keys, switch=None, before=False):
    codes = query.codes()
    if switch is not None:
        codes = jnp.where(switch, codes, -1.0)
    queries = query.rows()
    best = [None] * (query.count // LANES)
    merged = len(keys) > 1 and all(key.count < 2 * LANES for key in keys)
    pieces = [keys] if merged else [[key] for key in keys]
    for piece in pieces:
        rows = jnp.concatenate([key.rows() for key in piece], axis=0) if merged else piece[0].rows()
        columns = [key.columns() for key in piece]
        columns = jnp.concatenate(columns, axis=0) if merged else columns[0]
        count = rows.shape[0]
        scores = lax.dot_general(
            rows, queries, (((1,), (1,)), ((), ())), preferred_element_type=jnp.float32
        )
        for b in range(query.count // LANES):
            span = slice(b * LANES, (b + 1) * LANES)
            allowed = columns == codes[:, span]
            if before:
                key_at = lax.broadcasted_iota(jnp.int32, (count, LANES), 0)
                query_at = lax.broadcasted_iota(jnp.int32, (count, LANES), 1) + b * LANES
                allowed = allowed & (key_at < query_at)
            kept = jnp.where(allowed, scores[:, span], -1.0)
            part = jnp.max(kept.reshape(count // 8, 8, LANES), axis=0)
            best[b] = part if best[b] is None else jnp.maximum(best[b], part)
    for b, part in enumerate(best):
        span = slice(low + b * LANES, low + (b + 1) * LANES)
        line = jnp.max(part, axis=0, keepdims=True)
        out_ref[:, span] = jnp.maximum(out_ref[:, span], line)


def raise_all(outs, queries, keys):
    for out_ref, blocks in zip(outs, queries):
        for block in blocks:
            raise_best(out_ref, block.low, block, keys)


def place():
    index = lax.axis_index("wide")
    return index // 4, (index // 2) % 2, index % 2


def own_kernel(mine_ref, twin_ref, out_ref):
    core = place()[2]
    out_ref[...] = jnp.full(out_ref.shape, -1.0, jnp.float32)
    mine = whole(mine_ref)[0]
    raise_best(out_ref, 0, mine, whole(mine_ref), before=True)

    @pl.when(core == 1)
    def _():
        raise_best(out_ref, 0, mine, whole(twin_ref))


def here_kernel(
    own_ref, mine_ref, twin_ref, side_ref, side_low_ref, ridge_ref, ridge_twin_ref,
    head_ref, head_twin_ref, tail_ref, tail_twin_ref, mine_out, side_out, above_out,
):
    layer, column, _ = place()
    mine_out[...] = own_ref[...]
    for ref in (side_out, above_out):
        ref[...] = jnp.full(ref.shape, -1.0, jnp.float32)
    near = [whole(mine_ref), paired(side_ref, side_low_ref)]

    @pl.when(column == 0)
    def _():
        raise_all([side_out], near[1:], whole(mine_ref) + whole(twin_ref))

    @pl.when(layer % 2 == 1)
    def _():
        keys = split(head_ref, tail_ref) + split(head_twin_ref, tail_twin_ref)
        raise_all([mine_out, side_out], near, keys)

    @pl.when(layer == 2)
    def _():
        keys = whole(ridge_ref) + whole(ridge_twin_ref)
        above = split(head_ref, tail_ref)
        raise_all([mine_out, side_out, above_out], near + [above], keys)


VIEWS = {
    "whole": whole,
    "split": split,
    "halves": halves,
    "paired": paired,
    "end": lambda head_ref, tail_ref: split(head_ref, tail_ref)[1:],
    "low": lambda upper_ref, lower_ref: halves(upper_ref, lower_ref)[1:],
}


def seen(views, refs):
    listed = []
    for view, count in views:
        listed.append(VIEWS[view](*refs[:count]))
        refs = refs[count:]
    return listed, refs


def deep_kernel(queries, keys, started, worker, *refs):
    layer = place()[0]
    begun, refs = (refs[: len(queries)], refs[len(queries) :]) if started else ((), refs)
    query_blocks, refs = seen(queries, refs)
    key_blocks, outs = seen(keys, refs)
    for at, ref in enumerate(outs):
        ref[...] = begun[at][...] if started else jnp.full(ref.shape, -1.0, jnp.float32)

    @pl.when(layer == worker)
    def _():
        raise_all(outs, query_blocks, [block for blocks in key_blocks for block in blocks])


def scored(body, outputs, pairs, *arrays):
    width = arrays[-1].shape[1]
    return pl.pallas_call(
        body,
        out_shape=[pltpu.VMEM((1, count), jnp.float32) for count in outputs],
        in_specs=[pl.BlockSpec(memory_space=pltpu.VMEM)] * len(arrays),
        cost_estimate=pl.CostEstimate(
            flops=2 * pairs * width,
            transcendentals=0,
            bytes_accessed=sum(value.nbytes for value in arrays),
        ),
        compiler_params=PARAMS,
    )(*[pltpu.with_memory_space_constraint(value, pltpu.VMEM) for value in arrays])


def deepened(begun, queries, keys, worker=2):
    def views(blocks):
        return tuple((view, len(arrays)) for view, *arrays in blocks)

    rows = [sum(value.shape[0] for value in arrays) // LANES * LANES for _, *arrays in queries]
    ends = [arrays[-1].shape[0] // LANES * LANES for _, *arrays in keys]
    started = begun is not None
    body = functools.partial(deep_kernel, views(queries), views(keys), started, worker)
    arrays = [value for _, *values in (*queries, *keys) for value in values]
    pairs = sum(rows) * sum(ends)
    return scored(body, rows, pairs, *(begun if started else ()), *arrays)


def layered(embeddings, cluster_id):
    rows = embeddings.shape[0]
    spots = [(z, x, c) for z in range(LAYERS) for x in range(2) for c in range(2)]

    def hops(move):
        def at(z, x, c):
            return (z * 2 + x) * 2 + c

        return [(at(*spot), at(*move(*spot))) for spot in spots]

    across = hops(lambda z, x, c: (z, 1 - x, c))
    beside = hops(lambda z, x, c: (z, x, 1 - c))
    outer = hops(lambda z, x, c: (z ^ 1, x, c))
    inner = hops(lambda z, x, c: (z, x, 1 - c) if z in (0, 3) else (3 - z, x, c))
    cross = hops(lambda z, x, c: (z if z in (0, 3) else 3 - z, x, 1 - c))
    lift = [hop for hop in outer if hop[0] // 4 == 2]
    tilt = [(source, target ^ 2) for source, target in lift]

    def sent(value, pairs):
        return lax.ppermute(value, "wide", pairs)

    raw_ridge = sent(embeddings, inner)
    mine, head, tail, low, marks = tagged(embeddings, cluster_id[:, 0])
    near_head = sent(head, outer)
    side_low = sent(low, across)
    near_tail = sent(tail, outer)
    side = sent(head, across)
    twin = sent(mine, beside)
    ridge = arrived(raw_ridge, sent(marks, inner))
    deep_head = sent(near_head, inner)
    upper = sent(near_head[: rows // 2], across)
    lower = sent(side_low, outer)
    near_head_twin = sent(near_head, beside)
    deep_tail = sent(near_tail, inner)
    near_tail_twin = sent(near_tail, beside)
    ridge_twin = sent(ridge, beside)
    deep_head_twin = sent(deep_head, beside)
    deep_tail_twin = sent(deep_tail, beside)

    square = rows * rows
    (own,) = scored(own_kernel, [rows], 2 * square, mine, twin)
    best = scored(
        here_kernel, [rows] * 3, 8 * square,
        own, mine, twin, side, side_low, ridge, ridge_twin, near_head, near_head_twin, near_tail, near_tail_twin,
    )
    flat = [("whole", mine), ("paired", side, side_low)]
    steep = [("split", near_head, near_tail), ("halves", upper, lower)]
    deep, deep_twin = ("whole", deep_head), ("whole", deep_head_twin)
    third, fourth = ("end", deep_head, deep_tail), ("end", deep_head_twin, deep_tail_twin)
    best = deepened(best, flat + steep[:1], [deep])
    best = deepened(best, flat + steep[:1], [deep_twin])
    keys = [("whole", ridge), ("whole", ridge_twin), deep, deep_twin]
    first, second = best[:2]
    from_side = sent(second, across)
    best = best[2:] + deepened(None, steep[1:], keys)
    ends = [("end", near_head, near_tail), ("low", upper, lower)]
    lent, lent_twin = deepened(None, keys[:2], ends, worker=1)
    from_lent = sent(lent, inner)
    from_twin = sent(lent_twin, cross)
    best = deepened(best, steep, [third])
    third, fourth = deepened(best, steep, [fourth])
    from_below = sent(third, lift)
    from_slant = sent(fourth, tilt)
    top = lax.axis_index("wide") // 4 == LAYERS - 1
    under = jnp.where(top, jnp.maximum(from_below, from_slant), -1.0)
    early = jnp.maximum(jnp.maximum(first, from_side), jnp.maximum(from_lent, from_twin))
    return jnp.maximum(early, under)[0]


def per_device(embeddings, cluster_id):
    if lax.axis_size("wide") == 4 * LAYERS:
        return layered(embeddings, cluster_id)
    return routed(embeddings, cluster_id)


def solution(mesh):
    placed = (P(("dom", "wide"), None), P(("dom", "wide"), None))
    return jax.shard_map(
        per_device, mesh=mesh, in_specs=placed, out_specs=P(("dom", "wide")), check_vma=False
    )
```

```python
import functools
import math

import jax
import jax.numpy as jnp
from jax import lax
from jax.experimental import pallas as pl
from jax.experimental.pallas import tpu as pltpu
from jax.sharding import PartitionSpec as P


def swapped(value, axis, bit):
    mask = 2**bit
    pairs = [(source, source ^ mask) for source in range(lax.axis_size(axis))]
    return lax.ppermute(value, axis, pairs)


def normalize(embedded):
    values = embedded.astype(jnp.float32)
    inverse = lax.rsqrt(jnp.mean(values * values, axis=1, keepdims=True) + 1e-06)
    return (values * inverse * (1.0 / math.sqrt(values.shape[1]))).astype(jnp.bfloat16)


def pair_scores(queries, key_rows):
    return jnp.einsum("qd,kd->qk", queries, key_rows, preferred_element_type=jnp.float32)


def masked_max(scores, allowed):
    return jnp.max(jnp.where(allowed, scores, -1.0), axis=1)


def routed(embeddings, cluster_id):
    axis_size = lax.axis_size("wide")
    rows_dev = embeddings.shape[0]
    feature_dim = embeddings.shape[1]
    clusters = axis_size // 2
    capacity = (5 * rows_dev + 2 * axis_size - 1) // (2 * axis_size)
    buffer_rows = axis_size * capacity
    unit_rows = normalize(embeddings)
    labels = cluster_id[:, 0]
    my_index = lax.axis_index("wide")
    my_flip = my_index % 2
    position = lax.iota(jnp.int32, rows_dev)
    same_cluster = labels[:, None] == labels[None, :]
    earlier = position[None, :] < position[:, None]
    local_rank = jnp.sum((same_cluster & earlier).astype(jnp.int32), axis=1)
    target = 2 * labels + (local_rank + my_flip) % 2
    slot_index = target * capacity + local_rank // 2
    outgoing = jnp.zeros((buffer_rows, feature_dim), jnp.bfloat16).at[slot_index].set(unit_rows)
    cluster_count = jnp.sum(
        (labels[:, None] == lax.iota(jnp.int32, clusters)[None, :]).astype(jnp.int32), axis=0
    )
    parity = lax.iota(jnp.int32, axis_size) % 2
    send_count = (jnp.repeat(cluster_count, 2) + 1 - (parity + my_flip) % 2) // 2
    outgoing_blocks = outgoing.reshape(axis_size, capacity, feature_dim)
    count_blocks = send_count.reshape(axis_size, 1)
    received, counts = (
        lax.all_to_all(outgoing_blocks, "wide", split_axis=0, concat_axis=0, tiled=True),
        lax.all_to_all(count_blocks, "wide", split_axis=0, concat_axis=0, tiled=True),
    )
    own_rows = received.reshape(buffer_rows, feature_dim)
    partner, partner_counts = swapped((own_rows, counts), "wide", 0)
    side_bit = my_index % 2
    slot_pos = lax.iota(jnp.int32, capacity)
    sources = lax.iota(jnp.int32, axis_size)
    base_key = (sources[:, None] * (2 * capacity) + 2 * slot_pos[None, :]).reshape(-1)
    source_parity = jnp.repeat(sources % 2, capacity)
    own_key = base_key + (side_bit + source_parity) % 2
    partner_key = base_key + (1 - side_bit + source_parity) % 2
    own_live = (slot_pos[None, :] < counts).reshape(-1)
    partner_live = (slot_pos[None, :] < partner_counts).reshape(-1)
    blocks = 8
    query_rows = own_rows.reshape(blocks, -1, feature_dim)
    query_key = own_key.reshape(blocks, -1)

    def self_max(pieces):
        queries, keys_here = pieces
        return masked_max(
            pair_scores(queries, own_rows),
            own_live[None, :] & (own_key[None, :] < keys_here[:, None]),
        )

    self_best = lax.map(self_max, (query_rows, query_key)).reshape(-1)
    first = side_bit == 0
    left_rows = jnp.where(first, own_rows, partner)
    left_key = jnp.where(first, own_key, partner_key)
    left_live = jnp.where(first, own_live, partner_live)
    right_rows = jnp.where(first, partner, own_rows)
    right_key = jnp.where(first, partner_key, own_key)
    right_live = jnp.where(first, partner_live, own_live)
    half_rows = buffer_rows // 2
    start = side_bit * half_rows
    lower_rows = lax.dynamic_slice_in_dim(left_rows, start, half_rows, 0).reshape(
        blocks // 2, -1, feature_dim
    )
    lower_key = lax.dynamic_slice_in_dim(left_key, start, half_rows, 0).reshape(blocks // 2, -1)
    lower_live = lax.dynamic_slice_in_dim(left_live, start, half_rows, 0).reshape(blocks // 2, -1)

    def cross_max(pieces):
        queries, keys_here, live_here = pieces
        scores = pair_scores(queries, right_rows)
        row_best = masked_max(
            scores, right_live[None, :] & (right_key[None, :] < keys_here[:, None])
        )
        column_mask = live_here[:, None] & (keys_here[:, None] < right_key[None, :])
        column_best = jnp.max(jnp.where(column_mask, scores, -1.0), axis=0)
        return (row_best, column_best)

    row_best, column_best = lax.map(cross_max, (lower_rows, lower_key, lower_live))
    row_best = row_best.reshape(-1)
    column_best = jnp.max(column_best, axis=0)
    placed = lax.dynamic_update_slice_in_dim(
        jnp.full((buffer_rows,), -1.0, jnp.float32), row_best, start, 0
    )
    kept = jnp.where(first, placed, column_best)
    handed = jnp.where(first, column_best, placed)
    returned = swapped(handed, "wide", 0)
    best_all = jnp.maximum(self_best, jnp.maximum(kept, returned))
    back = lax.all_to_all(
        best_all.reshape(axis_size, capacity), "wide", split_axis=0, concat_axis=0, tiled=True
    )
    return back.reshape(-1)[slot_index]


LAYERS = 4
TAG_ROWS = 8
LANES = 128
PARAMS = pltpu.CompilerParams(vmem_limit_bytes=16 * 1024 * 1024)


def unit_of(rows):
    values = rows.astype(jnp.float32)
    inverse = lax.rsqrt(jnp.mean(values * values, axis=1, keepdims=True) + 1e-06)
    return (values * inverse * (1.0 / math.sqrt(rows.shape[1]))).astype(jnp.bfloat16)


def tag_kernel(
    rows_hbm, label_hbm, whole_ref, head_ref, tail_ref, low_ref, mark_ref, rows_ref, label_ref, done
):
    rows, width = rows_ref.shape
    cut = head_ref.shape[0] - TAG_ROWS
    spans = [(low, low + rows // 4) for low in range(0, rows, rows // 4)]
    labels = pltpu.make_async_copy(label_hbm, label_ref, done.at[len(spans)])
    labels.start()
    copies = []
    for at, (low, high) in enumerate(spans):
        part = pl.ds(low, high - low)
        copies.append(pltpu.make_async_copy(rows_hbm.at[part], rows_ref.at[part], done.at[at]))
        copies[-1].start()
    labels.wait()
    codes = (label_ref[...] + 1).astype(jnp.float32)
    line = jnp.broadcast_to(codes, (TAG_ROWS, rows)).astype(jnp.bfloat16)
    mark_ref[...] = line
    for ref, count in ((whole_ref, rows), (head_ref, cut), (low_ref, rows - cut)):
        ref[count:, :rows] = line
        if rows < width:
            ref[count:, rows:] = jnp.zeros((TAG_ROWS, width - rows), jnp.bfloat16)
    for copy, (low, high) in zip(copies, spans):
        copy.wait()
        unit = unit_of(rows_ref[low:high, :])
        whole_ref[low:high, :] = unit
        if high <= cut:
            head_ref[low:high, :] = unit
        else:
            tail_ref[low - cut : high - cut, :] = unit
            low_ref[low - cut : high - cut, :] = unit


def tagged(embeddings, labels):
    rows, width = embeddings.shape
    labels = labels.reshape(1, rows)
    cut = rows // 2
    shapes = ((rows + TAG_ROWS, width), (cut + TAG_ROWS, width), (rows - cut, width))
    shapes += ((rows - cut + TAG_ROWS, width), (TAG_ROWS, rows))
    return pl.pallas_call(
        tag_kernel,
        out_shape=[pltpu.VMEM(shape, jnp.bfloat16) for shape in shapes],
        in_specs=[pl.BlockSpec(memory_space=pltpu.HBM)] * 2,
        scratch_shapes=[
            pltpu.VMEM((rows, width), jnp.bfloat16),
            pltpu.VMEM((1, rows), jnp.int32),
            pltpu.SemaphoreType.DMA((5,)),
        ],
        compiler_params=PARAMS,
        name="tagged",
    )(*[pltpu.with_memory_space_constraint(value, pltpu.HBM) for value in (embeddings, labels)])


def ridge_kernel(rows_ref, mark_ref, out_ref):
    rows, width = rows_ref.shape
    out_ref[:rows, :] = unit_of(rows_ref[...])
    out_ref[rows:, :rows] = mark_ref[...]
    if rows < width:
        out_ref[rows:, rows:] = jnp.zeros((TAG_ROWS, width - rows), jnp.bfloat16)


def arrived(rows, marks):
    count, width = rows.shape
    return pl.pallas_call(
        ridge_kernel,
        out_shape=pltpu.VMEM((count + TAG_ROWS, width), jnp.bfloat16),
        in_specs=[pl.BlockSpec(memory_space=pltpu.VMEM)] * 2,
        compiler_params=PARAMS,
        name="arrived",
    )(*[pltpu.with_memory_space_constraint(value, pltpu.VMEM) for value in (rows, marks)])


class Block:
    def __init__(self, rows_ref, tag_ref, low, count):
        self.rows_ref = rows_ref
        self.tag_ref = tag_ref
        self.low = low
        self.count = count

    def rows(self):
        return self.rows_ref[: self.count, :]

    def codes(self):
        tags = self.tag_ref[self.tag_ref.shape[0] - TAG_ROWS :, self.low : self.low + self.count]
        return tags.astype(jnp.float32)[:1]

    def columns(self):
        return jnp.transpose(jnp.broadcast_to(self.codes(), (LANES, self.count)))


def whole(ref):
    return [Block(ref, ref, 0, ref.shape[0] - TAG_ROWS)]


def split(head_ref, tail_ref):
    cut = head_ref.shape[0] - TAG_ROWS
    return [
        Block(head_ref, head_ref, 0, cut),
        Block(tail_ref, head_ref, cut, tail_ref.shape[0]),
    ]


def paired(head_ref, low_ref):
    cut = head_ref.shape[0] - TAG_ROWS
    count = low_ref.shape[0] - TAG_ROWS
    return [Block(head_ref, head_ref, 0, cut), Block(low_ref, low_ref, cut, count)]


def halves(upper_ref, lower_ref):
    count = upper_ref.shape[0]
    return [Block(upper_ref, lower_ref, 0, count), Block(lower_ref, lower_ref, count, count)]


def raise_best(out_ref, low, query, keys, switch=None, before=False):
    codes = query.codes()
    if switch is not None:
        codes = jnp.where(switch, codes, -1.0)
    queries = query.rows()
    best = [None] * (query.count // LANES)
    merged = len(keys) > 1 and all(key.count < 2 * LANES for key in keys)
    pieces = [keys] if merged else [[key] for key in keys]
    for piece in pieces:
        rows = jnp.concatenate([key.rows() for key in piece], axis=0) if merged else piece[0].rows()
        columns = [key.columns() for key in piece]
        columns = jnp.concatenate(columns, axis=0) if merged else columns[0]
        count = rows.shape[0]
        scores = lax.dot_general(
            rows, queries, (((1,), (1,)), ((), ())), preferred_element_type=jnp.float32
        )
        for b in range(query.count // LANES):
            span = slice(b * LANES, (b + 1) * LANES)
            allowed = columns == codes[:, span]
            if before:
                key_at = lax.broadcasted_iota(jnp.int32, (count, LANES), 0)
                query_at = lax.broadcasted_iota(jnp.int32, (count, LANES), 1) + b * LANES
                allowed = allowed & (key_at < query_at)
            kept = jnp.where(allowed, scores[:, span], -1.0)
            part = jnp.max(kept.reshape(count // 8, 8, LANES), axis=0)
            best[b] = part if best[b] is None else jnp.maximum(best[b], part)
    for b, part in enumerate(best):
        span = slice(low + b * LANES, low + (b + 1) * LANES)
        line = jnp.max(part, axis=0, keepdims=True)
        out_ref[:, span] = jnp.maximum(out_ref[:, span], line)


def raise_all(outs, queries, keys):
    for out_ref, blocks in zip(outs, queries):
        for block in blocks:
            raise_best(out_ref, block.low, block, keys)


def place():
    index = lax.axis_index("wide")
    return index // 4, (index // 2) % 2, index % 2


def own_kernel(mine_ref, twin_ref, out_ref):
    core = place()[2]
    out_ref[...] = jnp.full(out_ref.shape, -1.0, jnp.float32)
    mine = whole(mine_ref)[0]
    raise_best(out_ref, 0, mine, whole(mine_ref), before=True)

    @pl.when(core == 1)
    def _():
        raise_best(out_ref, 0, mine, whole(twin_ref))


def here_kernel(
    own_ref, mine_ref, twin_ref, side_ref, side_low_ref, ridge_ref, ridge_twin_ref,
    head_ref, head_twin_ref, tail_ref, tail_twin_ref, mine_out, side_out, above_out,
):
    layer, column, _ = place()
    mine_out[...] = own_ref[...]
    for ref in (side_out, above_out):
        ref[...] = jnp.full(ref.shape, -1.0, jnp.float32)
    near = [whole(mine_ref), paired(side_ref, side_low_ref)]

    @pl.when(column == 0)
    def _():
        raise_all([side_out], near[1:], whole(mine_ref) + whole(twin_ref))

    @pl.when(layer % 2 == 1)
    def _():
        keys = split(head_ref, tail_ref) + split(head_twin_ref, tail_twin_ref)
        raise_all([mine_out, side_out], near, keys)

    @pl.when(layer == 2)
    def _():
        keys = whole(ridge_ref) + whole(ridge_twin_ref)
        above = split(head_ref, tail_ref)
        raise_all([mine_out, side_out, above_out], near + [above], keys)


VIEWS = {
    "whole": whole,
    "split": split,
    "halves": halves,
    "paired": paired,
    "end": lambda head_ref, tail_ref: split(head_ref, tail_ref)[1:],
    "first": lambda head_ref, spare_ref: whole(head_ref),
    "low": lambda upper_ref, lower_ref: halves(upper_ref, lower_ref)[1:],
}


def seen(views, refs):
    listed = []
    for view, count in views:
        listed.append(VIEWS[view](*refs[:count]))
        refs = refs[count:]
    return listed, refs


def deep_kernel(queries, keys, started, worker, *refs):
    layer = place()[0]
    begun, refs = (refs[: len(queries)], refs[len(queries) :]) if started else ((), refs)
    query_blocks, refs = seen(queries, refs)
    key_blocks, outs = seen(keys, refs)
    for at, ref in enumerate(outs):
        ref[...] = begun[at][...] if started else jnp.full(ref.shape, -1.0, jnp.float32)

    @pl.when(layer == worker)
    def _():
        raise_all(outs, query_blocks, [block for blocks in key_blocks for block in blocks])


def scored(body, outputs, pairs, *arrays):
    width = arrays[-1].shape[1]
    return pl.pallas_call(
        body,
        out_shape=[pltpu.VMEM((1, count), jnp.float32) for count in outputs],
        in_specs=[pl.BlockSpec(memory_space=pltpu.VMEM)] * len(arrays),
        cost_estimate=pl.CostEstimate(
            flops=2 * pairs * width,
            transcendentals=0,
            bytes_accessed=sum(value.nbytes for value in arrays),
        ),
        compiler_params=PARAMS,
    )(*[pltpu.with_memory_space_constraint(value, pltpu.VMEM) for value in arrays])


def deepened(begun, queries, keys, worker=2):
    def views(blocks):
        return tuple((view, len(arrays)) for view, *arrays in blocks)

    rows = [sum(value.shape[0] for value in arrays) // LANES * LANES for _, *arrays in queries]
    ends = [arrays[-1].shape[0] // LANES * LANES for _, *arrays in keys]
    started = begun is not None
    body = functools.partial(deep_kernel, views(queries), views(keys), started, worker)
    arrays = [value for _, *values in (*queries, *keys) for value in values]
    pairs = sum(rows) * sum(ends)
    return scored(body, rows, pairs, *(begun if started else ()), *arrays)


def layered(embeddings, cluster_id):
    rows = embeddings.shape[0]
    spots = [(z, x, c) for z in range(LAYERS) for x in range(2) for c in range(2)]

    def hops(move):
        def at(z, x, c):
            return (z * 2 + x) * 2 + c

        return [(at(*spot), at(*move(*spot))) for spot in spots]

    across = hops(lambda z, x, c: (z, 1 - x, c))
    beside = hops(lambda z, x, c: (z, x, 1 - c))
    outer = hops(lambda z, x, c: (z ^ 1, x, c))
    inner = hops(lambda z, x, c: (z, x, 1 - c) if z in (0, 3) else (3 - z, x, c))
    slant = hops(lambda z, x, c: (z ^ 1, 1 - x, c))
    spring = hops(lambda z, x, c: ((z, x, 1 - c), (3, x, c), (1, x, c), (2, x, c))[z])

    def sent(value, pairs):
        return lax.ppermute(value, "wide", pairs)

    raw_ridge = sent(embeddings, inner)
    mine, head, tail, low, marks = tagged(embeddings, cluster_id[:, 0])
    near_head = sent(head, outer)
    side_low = sent(low, across)
    near_tail = sent(tail, outer)
    side = sent(head, across)
    twin = sent(mine, beside)
    ridge = arrived(raw_ridge, sent(marks, inner))
    deep_head = sent(near_head, inner)
    upper = sent(near_head[: rows // 2], across)
    lower = sent(side_low, outer)
    near_head_twin = sent(near_head, beside)
    deep_tail = sent(near_tail, inner)
    near_tail_twin = sent(near_tail, beside)
    ridge_twin = sent(ridge, beside)
    deep_head_twin = sent(deep_head, beside)
    lower_twin = sent(lower, beside)

    square = rows * rows
    (own,) = scored(own_kernel, [rows], 2 * square, mine, twin)
    best = scored(
        here_kernel, [rows] * 3, 8 * square,
        own, mine, twin, side, side_low, ridge, ridge_twin, near_head, near_head_twin, near_tail, near_tail_twin,
    )
    flat = [("whole", mine), ("paired", side, side_low)]
    steep = [("split", near_head, near_tail), ("halves", upper, lower)]
    deep, deep_twin = ("whole", deep_head), ("whole", deep_head_twin)
    best = deepened(best, flat + steep[:1], [deep])
    best = deepened(best, flat + steep[:1], [deep_twin])
    keys = [("whole", ridge), ("whole", ridge_twin), deep, deep_twin]
    first, second = best[:2]
    from_side = sent(second, across)
    third, fourth = best[2:] + deepened(None, steep[1:], keys)
    from_below = sent(third, outer)
    from_far = sent(fourth, slant)
    ends = [
        ("end", near_head, near_tail), ("end", near_head_twin, near_tail_twin),
        ("low", upper, lower), ("low", upper, lower_twin),
    ]
    guests = [("whole", ridge), ("first", deep_head, near_tail)]
    begun = deepened(None, guests, ends[:2], worker=1)
    lent, lifted = deepened(begun, guests, ends[2:], worker=1)
    (lifted,) = deepened([lifted], [("end", deep_head, deep_tail)], ends, worker=1)
    from_lifted = sent(lifted, spring)
    from_lent = sent(lent, inner)
    parts = (first, from_side, from_below, from_far, from_lent, from_lifted)
    return functools.reduce(jnp.maximum, parts)[0]


def per_device(embeddings, cluster_id):
    if lax.axis_size("wide") == 4 * LAYERS:
        return layered(embeddings, cluster_id)
    return routed(embeddings, cluster_id)


def solution(mesh):
    placed = (P(("dom", "wide"), None), P(("dom", "wide"), None))
    return jax.shard_map(
        per_device, mesh=mesh, in_specs=placed, out_specs=P(("dom", "wide")), check_vma=False
    )
```

```python
import functools
import math

import jax
import jax.numpy as jnp
from jax import lax
from jax.experimental import pallas as pl
from jax.experimental.pallas import tpu as pltpu
from jax.sharding import PartitionSpec as P


def swapped(value, axis, bit):
    mask = 2**bit
    pairs = [(source, source ^ mask) for source in range(lax.axis_size(axis))]
    return lax.ppermute(value, axis, pairs)


def normalize(embedded):
    values = embedded.astype(jnp.float32)
    inverse = lax.rsqrt(jnp.mean(values * values, axis=1, keepdims=True) + 1e-06)
    return (values * inverse * (1.0 / math.sqrt(values.shape[1]))).astype(jnp.bfloat16)


def pair_scores(queries, key_rows):
    return jnp.einsum("qd,kd->qk", queries, key_rows, preferred_element_type=jnp.float32)


def masked_max(scores, allowed):
    return jnp.max(jnp.where(allowed, scores, -1.0), axis=1)


def routed(embeddings, cluster_id):
    axis_size = lax.axis_size("wide")
    rows_dev = embeddings.shape[0]
    feature_dim = embeddings.shape[1]
    clusters = axis_size // 2
    capacity = (5 * rows_dev + 2 * axis_size - 1) // (2 * axis_size)
    buffer_rows = axis_size * capacity
    unit_rows = normalize(embeddings)
    labels = cluster_id[:, 0]
    my_index = lax.axis_index("wide")
    my_flip = my_index % 2
    position = lax.iota(jnp.int32, rows_dev)
    same_cluster = labels[:, None] == labels[None, :]
    earlier = position[None, :] < position[:, None]
    local_rank = jnp.sum((same_cluster & earlier).astype(jnp.int32), axis=1)
    target = 2 * labels + (local_rank + my_flip) % 2
    slot_index = target * capacity + local_rank // 2
    outgoing = jnp.zeros((buffer_rows, feature_dim), jnp.bfloat16).at[slot_index].set(unit_rows)
    cluster_count = jnp.sum(
        (labels[:, None] == lax.iota(jnp.int32, clusters)[None, :]).astype(jnp.int32), axis=0
    )
    parity = lax.iota(jnp.int32, axis_size) % 2
    send_count = (jnp.repeat(cluster_count, 2) + 1 - (parity + my_flip) % 2) // 2
    outgoing_blocks = outgoing.reshape(axis_size, capacity, feature_dim)
    count_blocks = send_count.reshape(axis_size, 1)
    received, counts = (
        lax.all_to_all(outgoing_blocks, "wide", split_axis=0, concat_axis=0, tiled=True),
        lax.all_to_all(count_blocks, "wide", split_axis=0, concat_axis=0, tiled=True),
    )
    own_rows = received.reshape(buffer_rows, feature_dim)
    partner, partner_counts = swapped((own_rows, counts), "wide", 0)
    side_bit = my_index % 2
    slot_pos = lax.iota(jnp.int32, capacity)
    sources = lax.iota(jnp.int32, axis_size)
    base_key = (sources[:, None] * (2 * capacity) + 2 * slot_pos[None, :]).reshape(-1)
    source_parity = jnp.repeat(sources % 2, capacity)
    own_key = base_key + (side_bit + source_parity) % 2
    partner_key = base_key + (1 - side_bit + source_parity) % 2
    own_live = (slot_pos[None, :] < counts).reshape(-1)
    partner_live = (slot_pos[None, :] < partner_counts).reshape(-1)
    blocks = 8
    query_rows = own_rows.reshape(blocks, -1, feature_dim)
    query_key = own_key.reshape(blocks, -1)

    def self_max(pieces):
        queries, keys_here = pieces
        return masked_max(
            pair_scores(queries, own_rows),
            own_live[None, :] & (own_key[None, :] < keys_here[:, None]),
        )

    self_best = lax.map(self_max, (query_rows, query_key)).reshape(-1)
    first = side_bit == 0
    left_rows = jnp.where(first, own_rows, partner)
    left_key = jnp.where(first, own_key, partner_key)
    left_live = jnp.where(first, own_live, partner_live)
    right_rows = jnp.where(first, partner, own_rows)
    right_key = jnp.where(first, partner_key, own_key)
    right_live = jnp.where(first, partner_live, own_live)
    half_rows = buffer_rows // 2
    start = side_bit * half_rows
    lower_rows = lax.dynamic_slice_in_dim(left_rows, start, half_rows, 0).reshape(
        blocks // 2, -1, feature_dim
    )
    lower_key = lax.dynamic_slice_in_dim(left_key, start, half_rows, 0).reshape(blocks // 2, -1)
    lower_live = lax.dynamic_slice_in_dim(left_live, start, half_rows, 0).reshape(blocks // 2, -1)

    def cross_max(pieces):
        queries, keys_here, live_here = pieces
        scores = pair_scores(queries, right_rows)
        row_best = masked_max(
            scores, right_live[None, :] & (right_key[None, :] < keys_here[:, None])
        )
        column_mask = live_here[:, None] & (keys_here[:, None] < right_key[None, :])
        column_best = jnp.max(jnp.where(column_mask, scores, -1.0), axis=0)
        return (row_best, column_best)

    row_best, column_best = lax.map(cross_max, (lower_rows, lower_key, lower_live))
    row_best = row_best.reshape(-1)
    column_best = jnp.max(column_best, axis=0)
    placed = lax.dynamic_update_slice_in_dim(
        jnp.full((buffer_rows,), -1.0, jnp.float32), row_best, start, 0
    )
    kept = jnp.where(first, placed, column_best)
    handed = jnp.where(first, column_best, placed)
    returned = swapped(handed, "wide", 0)
    best_all = jnp.maximum(self_best, jnp.maximum(kept, returned))
    back = lax.all_to_all(
        best_all.reshape(axis_size, capacity), "wide", split_axis=0, concat_axis=0, tiled=True
    )
    return back.reshape(-1)[slot_index]


LAYERS = 4
TAG_ROWS = 8
LANES = 128
PARAMS = pltpu.CompilerParams(vmem_limit_bytes=16 * 1024 * 1024)


def unit_of(rows):
    values = rows.astype(jnp.float32)
    inverse = lax.rsqrt(jnp.mean(values * values, axis=1, keepdims=True) + 1e-06)
    return (values * inverse * (1.0 / math.sqrt(rows.shape[1]))).astype(jnp.bfloat16)


def tag_kernel(
    rows_hbm, label_hbm, whole_ref, head_ref, tail_ref, low_ref, mark_ref, rows_ref, label_ref, done
):
    rows, width = rows_ref.shape
    cut = head_ref.shape[0] - TAG_ROWS
    spans = [(low, low + rows // 4) for low in range(0, rows, rows // 4)]
    labels = pltpu.make_async_copy(label_hbm, label_ref, done.at[len(spans)])
    labels.start()
    copies = []
    for at, (low, high) in enumerate(spans):
        part = pl.ds(low, high - low)
        copies.append(pltpu.make_async_copy(rows_hbm.at[part], rows_ref.at[part], done.at[at]))
        copies[-1].start()
    labels.wait()
    codes = (label_ref[...] + 1).astype(jnp.float32)
    line = jnp.broadcast_to(codes, (TAG_ROWS, rows)).astype(jnp.bfloat16)
    mark_ref[...] = line
    for ref, count in ((whole_ref, rows), (head_ref, cut), (low_ref, rows - cut)):
        ref[count:, :rows] = line
        if rows < width:
            ref[count:, rows:] = jnp.zeros((TAG_ROWS, width - rows), jnp.bfloat16)
    for copy, (low, high) in zip(copies, spans):
        copy.wait()
        unit = unit_of(rows_ref[low:high, :])
        whole_ref[low:high, :] = unit
        if high <= cut:
            head_ref[low:high, :] = unit
        else:
            tail_ref[low - cut : high - cut, :] = unit
            low_ref[low - cut : high - cut, :] = unit


def tagged(embeddings, labels):
    rows, width = embeddings.shape
    labels = labels.reshape(1, rows)
    cut = rows // 2
    shapes = ((rows + TAG_ROWS, width), (cut + TAG_ROWS, width), (rows - cut, width))
    shapes += ((rows - cut + TAG_ROWS, width), (TAG_ROWS, rows))
    return pl.pallas_call(
        tag_kernel,
        out_shape=[pltpu.VMEM(shape, jnp.bfloat16) for shape in shapes],
        in_specs=[pl.BlockSpec(memory_space=pltpu.HBM)] * 2,
        scratch_shapes=[
            pltpu.VMEM((rows, width), jnp.bfloat16),
            pltpu.VMEM((1, rows), jnp.int32),
            pltpu.SemaphoreType.DMA((5,)),
        ],
        compiler_params=PARAMS,
        name="tagged",
    )(*[pltpu.with_memory_space_constraint(value, pltpu.HBM) for value in (embeddings, labels)])


def ridge_kernel(rows_ref, mark_ref, out_ref):
    rows, width = rows_ref.shape
    out_ref[:rows, :] = unit_of(rows_ref[...])
    out_ref[rows:, :rows] = mark_ref[...]
    if rows < width:
        out_ref[rows:, rows:] = jnp.zeros((TAG_ROWS, width - rows), jnp.bfloat16)


def arrived(rows, marks):
    count, width = rows.shape
    return pl.pallas_call(
        ridge_kernel,
        out_shape=pltpu.VMEM((count + TAG_ROWS, width), jnp.bfloat16),
        in_specs=[pl.BlockSpec(memory_space=pltpu.VMEM)] * 2,
        compiler_params=PARAMS,
        name="arrived",
    )(*[pltpu.with_memory_space_constraint(value, pltpu.VMEM) for value in (rows, marks)])


class Block:
    def __init__(self, rows_ref, tag_ref, low, count):
        self.rows_ref = rows_ref
        self.tag_ref = tag_ref
        self.low = low
        self.count = count

    def rows(self):
        return self.rows_ref[: self.count, :]

    def codes(self):
        tags = self.tag_ref[self.tag_ref.shape[0] - TAG_ROWS :, self.low : self.low + self.count]
        return tags.astype(jnp.float32)[:1]

    def columns(self):
        return jnp.transpose(jnp.broadcast_to(self.codes(), (LANES, self.count)))


def whole(ref):
    return [Block(ref, ref, 0, ref.shape[0] - TAG_ROWS)]


def split(head_ref, tail_ref):
    cut = head_ref.shape[0] - TAG_ROWS
    return [
        Block(head_ref, head_ref, 0, cut),
        Block(tail_ref, head_ref, cut, tail_ref.shape[0]),
    ]


def paired(head_ref, low_ref):
    cut = head_ref.shape[0] - TAG_ROWS
    count = low_ref.shape[0] - TAG_ROWS
    return [Block(head_ref, head_ref, 0, cut), Block(low_ref, low_ref, cut, count)]


def halves(upper_ref, lower_ref):
    count = upper_ref.shape[0]
    return [Block(upper_ref, lower_ref, 0, count), Block(lower_ref, lower_ref, count, count)]


def raise_best(out_ref, low, query, keys, switch=None, before=False):
    codes = query.codes()
    if switch is not None:
        codes = jnp.where(switch, codes, -1.0)
    queries = query.rows()
    best = [None] * (query.count // LANES)
    merged = len(keys) > 1 and all(key.count < 2 * LANES for key in keys)
    pieces = [keys] if merged else [[key] for key in keys]
    for piece in pieces:
        rows = jnp.concatenate([key.rows() for key in piece], axis=0) if merged else piece[0].rows()
        columns = [key.columns() for key in piece]
        columns = jnp.concatenate(columns, axis=0) if merged else columns[0]
        count = rows.shape[0]
        scores = lax.dot_general(
            rows, queries, (((1,), (1,)), ((), ())), preferred_element_type=jnp.float32
        )
        for b in range(query.count // LANES):
            span = slice(b * LANES, (b + 1) * LANES)
            allowed = columns == codes[:, span]
            if before:
                key_at = lax.broadcasted_iota(jnp.int32, (count, LANES), 0)
                query_at = lax.broadcasted_iota(jnp.int32, (count, LANES), 1) + b * LANES
                allowed = allowed & (key_at < query_at)
            kept = jnp.where(allowed, scores[:, span], -1.0)
            part = jnp.max(kept.reshape(count // 8, 8, LANES), axis=0)
            best[b] = part if best[b] is None else jnp.maximum(best[b], part)
    for b, part in enumerate(best):
        span = slice(low + b * LANES, low + (b + 1) * LANES)
        line = jnp.max(part, axis=0, keepdims=True)
        out_ref[:, span] = jnp.maximum(out_ref[:, span], line)


def raise_all(outs, queries, keys):
    for out_ref, blocks in zip(outs, queries):
        for block in blocks:
            raise_best(out_ref, block.low, block, keys)


def place():
    index = lax.axis_index("wide")
    return index // 4, (index // 2) % 2, index % 2


def own_kernel(mine_ref, twin_ref, out_ref):
    core = place()[2]
    out_ref[...] = jnp.full(out_ref.shape, -1.0, jnp.float32)
    mine = whole(mine_ref)[0]
    raise_best(out_ref, 0, mine, whole(mine_ref), before=True)

    @pl.when(core == 1)
    def _():
        raise_best(out_ref, 0, mine, whole(twin_ref))


def here_kernel(
    own_ref, mine_ref, twin_ref, side_ref, side_low_ref, ridge_ref, ridge_twin_ref,
    head_ref, tail_ref, mine_out, side_out, above_out,
):
    layer, column, _ = place()
    mine_out[...] = own_ref[...]
    for ref in (side_out, above_out):
        ref[...] = jnp.full(ref.shape, -1.0, jnp.float32)
    near = [whole(mine_ref), paired(side_ref, side_low_ref)]

    @pl.when(column == 0)
    def _():
        raise_all([side_out], near[1:], whole(mine_ref) + whole(twin_ref))

    @pl.when(layer == 2)
    def _():
        keys = whole(ridge_ref) + whole(ridge_twin_ref)
        above = split(head_ref, tail_ref)
        raise_all([mine_out, side_out, above_out], near + [above], keys)


VIEWS = {
    "whole": whole,
    "split": split,
    "halves": halves,
    "paired": paired,
    "end": lambda head_ref, tail_ref: split(head_ref, tail_ref)[1:],
    "first": lambda head_ref, spare_ref: whole(head_ref),
    "low": lambda upper_ref, lower_ref: halves(upper_ref, lower_ref)[1:],
}


def seen(views, refs):
    listed = []
    for view, count in views:
        listed.append(VIEWS[view](*refs[:count]))
        refs = refs[count:]
    return listed, refs


def deep_kernel(queries, keys, started, worker, *refs):
    layer = place()[0]
    begun, refs = (refs[: len(queries)], refs[len(queries) :]) if started else ((), refs)
    query_blocks, refs = seen(queries, refs)
    key_blocks, outs = seen(keys, refs)
    for at, ref in enumerate(outs):
        ref[...] = begun[at][...] if started else jnp.full(ref.shape, -1.0, jnp.float32)

    @pl.when((layer == worker) if worker else (layer % 2 == 1))
    def _():
        raise_all(outs, query_blocks, [block for blocks in key_blocks for block in blocks])


def scored(body, outputs, pairs, *arrays):
    width = arrays[-1].shape[1]
    return pl.pallas_call(
        body,
        out_shape=[pltpu.VMEM((1, count), jnp.float32) for count in outputs],
        in_specs=[pl.BlockSpec(memory_space=pltpu.VMEM)] * len(arrays),
        cost_estimate=pl.CostEstimate(
            flops=2 * pairs * width,
            transcendentals=0,
            bytes_accessed=sum(value.nbytes for value in arrays),
        ),
        compiler_params=PARAMS,
    )(*[pltpu.with_memory_space_constraint(value, pltpu.VMEM) for value in arrays])


def deepened(begun, queries, keys, worker=2):
    def views(blocks):
        return tuple((view, len(arrays)) for view, *arrays in blocks)

    rows = [sum(value.shape[0] for value in arrays) // LANES * LANES for _, *arrays in queries]
    ends = [arrays[-1].shape[0] // LANES * LANES for _, *arrays in keys]
    started = begun is not None
    body = functools.partial(deep_kernel, views(queries), views(keys), started, worker)
    arrays = [value for _, *values in (*queries, *keys) for value in values]
    pairs = sum(rows) * sum(ends)
    return scored(body, rows, pairs, *(begun if started else ()), *arrays)


def layered(embeddings, cluster_id):
    rows = embeddings.shape[0]
    spots = [(z, x, c) for z in range(LAYERS) for x in range(2) for c in range(2)]

    def hops(move):
        def at(z, x, c):
            return (z * 2 + x) * 2 + c

        return [(at(*spot), at(*move(*spot))) for spot in spots]

    across = hops(lambda z, x, c: (z, 1 - x, c))
    beside = hops(lambda z, x, c: (z, x, 1 - c))
    outer = hops(lambda z, x, c: (z ^ 1, x, c))
    inner = hops(lambda z, x, c: (z, x, 1 - c) if z in (0, 3) else (3 - z, x, c))
    slant = hops(lambda z, x, c: (z ^ 1, 1 - x, c))
    spring = hops(lambda z, x, c: ((z, x, 1 - c), (3, x, c), (1, x, c), (2, x, c))[z])

    def sent(value, pairs):
        return lax.ppermute(value, "wide", pairs)

    raw_ridge = sent(embeddings, inner)
    mine, head, tail, low, marks = tagged(embeddings, cluster_id[:, 0])
    near_head = sent(head, outer)
    side_low = sent(low, across)
    near_tail = sent(tail, outer)
    side = sent(head, across)
    twin = sent(mine, beside)
    ridge = arrived(raw_ridge, sent(marks, inner))
    deep_head = sent(near_head, inner)
    upper = sent(near_head[: rows // 2], across)
    lower = sent(side_low, outer)
    near_head_twin = sent(near_head, beside)
    deep_tail = sent(near_tail, inner)
    near_tail_twin = sent(near_tail, beside)
    ridge_twin = sent(ridge, beside)
    deep_head_twin = sent(deep_head, beside)
    lower_twin = sent(lower, beside)

    square = rows * rows
    (own,) = scored(own_kernel, [rows], 2 * square, mine, twin)
    best = scored(
        here_kernel, [rows] * 3, 8 * square,
        own, mine, twin, side, side_low, ridge, ridge_twin, near_head, near_tail,
    )
    flat = [("whole", mine), ("paired", side, side_low)]
    steep = [("split", near_head, near_tail), ("halves", upper, lower)]
    layers = [("split", near_head, near_tail), ("split", near_head_twin, near_tail_twin)]
    best = deepened(best[:2], flat, layers, worker=None) + best[2:]
    deep, deep_twin = ("whole", deep_head), ("whole", deep_head_twin)
    best = deepened(best, flat + steep[:1], [deep])
    best = deepened(best, flat + steep[:1], [deep_twin])
    keys = [("whole", ridge), ("whole", ridge_twin), deep, deep_twin]
    first, second = best[:2]
    from_side = sent(second, across)
    third, fourth = best[2:] + deepened(None, steep[1:], keys)
    from_below = sent(third, outer)
    from_far = sent(fourth, slant)
    ends = [
        ("end", near_head, near_tail), ("end", near_head_twin, near_tail_twin),
        ("low", upper, lower), ("low", upper, lower_twin),
    ]
    guests = [("whole", ridge), ("first", deep_head, near_tail)]
    begun = deepened(None, guests, ends[:2], worker=1)
    lent, lifted = deepened(begun, guests, ends[2:], worker=1)
    (lifted,) = deepened([lifted], [("end", deep_head, deep_tail)], ends, worker=1)
    from_lifted = sent(lifted, spring)
    from_lent = sent(lent, inner)
    parts = (first, from_side, from_below, from_far, from_lent, from_lifted)
    return functools.reduce(jnp.maximum, parts)[0]


def per_device(embeddings, cluster_id):
    if lax.axis_size("wide") == 4 * LAYERS:
        return layered(embeddings, cluster_id)
    return routed(embeddings, cluster_id)


def solution(mesh):
    placed = (P(("dom", "wide"), None), P(("dom", "wide"), None))
    return jax.shard_map(
        per_device, mesh=mesh, in_specs=placed, out_specs=P(("dom", "wide")), check_vma=False
    )
```

```python
import functools
import math

import jax
import jax.numpy as jnp
from jax import lax
from jax.experimental import pallas as pl
from jax.experimental.pallas import tpu as pltpu
from jax.sharding import PartitionSpec as P


def swapped(value, axis, bit):
    mask = 2**bit
    pairs = [(source, source ^ mask) for source in range(lax.axis_size(axis))]
    return lax.ppermute(value, axis, pairs)


def normalize(embedded):
    values = embedded.astype(jnp.float32)
    inverse = lax.rsqrt(jnp.mean(values * values, axis=1, keepdims=True) + 1e-06)
    return (values * inverse * (1.0 / math.sqrt(values.shape[1]))).astype(jnp.bfloat16)


def pair_scores(queries, key_rows):
    return jnp.einsum("qd,kd->qk", queries, key_rows, preferred_element_type=jnp.float32)


def masked_max(scores, allowed):
    return jnp.max(jnp.where(allowed, scores, -1.0), axis=1)


def routed(embeddings, cluster_id):
    axis_size = lax.axis_size("wide")
    rows_dev = embeddings.shape[0]
    feature_dim = embeddings.shape[1]
    clusters = axis_size // 2
    capacity = (5 * rows_dev + 2 * axis_size - 1) // (2 * axis_size)
    buffer_rows = axis_size * capacity
    unit_rows = normalize(embeddings)
    labels = cluster_id[:, 0]
    my_index = lax.axis_index("wide")
    my_flip = my_index % 2
    position = lax.iota(jnp.int32, rows_dev)
    same_cluster = labels[:, None] == labels[None, :]
    earlier = position[None, :] < position[:, None]
    local_rank = jnp.sum((same_cluster & earlier).astype(jnp.int32), axis=1)
    target = 2 * labels + (local_rank + my_flip) % 2
    slot_index = target * capacity + local_rank // 2
    outgoing = jnp.zeros((buffer_rows, feature_dim), jnp.bfloat16).at[slot_index].set(unit_rows)
    cluster_count = jnp.sum(
        (labels[:, None] == lax.iota(jnp.int32, clusters)[None, :]).astype(jnp.int32), axis=0
    )
    parity = lax.iota(jnp.int32, axis_size) % 2
    send_count = (jnp.repeat(cluster_count, 2) + 1 - (parity + my_flip) % 2) // 2
    outgoing_blocks = outgoing.reshape(axis_size, capacity, feature_dim)
    count_blocks = send_count.reshape(axis_size, 1)
    received, counts = (
        lax.all_to_all(outgoing_blocks, "wide", split_axis=0, concat_axis=0, tiled=True),
        lax.all_to_all(count_blocks, "wide", split_axis=0, concat_axis=0, tiled=True),
    )
    own_rows = received.reshape(buffer_rows, feature_dim)
    partner, partner_counts = swapped((own_rows, counts), "wide", 0)
    side_bit = my_index % 2
    slot_pos = lax.iota(jnp.int32, capacity)
    sources = lax.iota(jnp.int32, axis_size)
    base_key = (sources[:, None] * (2 * capacity) + 2 * slot_pos[None, :]).reshape(-1)
    source_parity = jnp.repeat(sources % 2, capacity)
    own_key = base_key + (side_bit + source_parity) % 2
    partner_key = base_key + (1 - side_bit + source_parity) % 2
    own_live = (slot_pos[None, :] < counts).reshape(-1)
    partner_live = (slot_pos[None, :] < partner_counts).reshape(-1)
    blocks = 8
    query_rows = own_rows.reshape(blocks, -1, feature_dim)
    query_key = own_key.reshape(blocks, -1)

    def self_max(pieces):
        queries, keys_here = pieces
        return masked_max(
            pair_scores(queries, own_rows),
            own_live[None, :] & (own_key[None, :] < keys_here[:, None]),
        )

    self_best = lax.map(self_max, (query_rows, query_key)).reshape(-1)
    first = side_bit == 0
    left_rows = jnp.where(first, own_rows, partner)
    left_key = jnp.where(first, own_key, partner_key)
    left_live = jnp.where(first, own_live, partner_live)
    right_rows = jnp.where(first, partner, own_rows)
    right_key = jnp.where(first, partner_key, own_key)
    right_live = jnp.where(first, partner_live, own_live)
    half_rows = buffer_rows // 2
    start = side_bit * half_rows
    lower_rows = lax.dynamic_slice_in_dim(left_rows, start, half_rows, 0).reshape(
        blocks // 2, -1, feature_dim
    )
    lower_key = lax.dynamic_slice_in_dim(left_key, start, half_rows, 0).reshape(blocks // 2, -1)
    lower_live = lax.dynamic_slice_in_dim(left_live, start, half_rows, 0).reshape(blocks // 2, -1)

    def cross_max(pieces):
        queries, keys_here, live_here = pieces
        scores = pair_scores(queries, right_rows)
        row_best = masked_max(
            scores, right_live[None, :] & (right_key[None, :] < keys_here[:, None])
        )
        column_mask = live_here[:, None] & (keys_here[:, None] < right_key[None, :])
        column_best = jnp.max(jnp.where(column_mask, scores, -1.0), axis=0)
        return (row_best, column_best)

    row_best, column_best = lax.map(cross_max, (lower_rows, lower_key, lower_live))
    row_best = row_best.reshape(-1)
    column_best = jnp.max(column_best, axis=0)
    placed = lax.dynamic_update_slice_in_dim(
        jnp.full((buffer_rows,), -1.0, jnp.float32), row_best, start, 0
    )
    kept = jnp.where(first, placed, column_best)
    handed = jnp.where(first, column_best, placed)
    returned = swapped(handed, "wide", 0)
    best_all = jnp.maximum(self_best, jnp.maximum(kept, returned))
    back = lax.all_to_all(
        best_all.reshape(axis_size, capacity), "wide", split_axis=0, concat_axis=0, tiled=True
    )
    return back.reshape(-1)[slot_index]


LAYERS = 4
TAG_ROWS = 8
LANES = 128
PARAMS = pltpu.CompilerParams(vmem_limit_bytes=16 * 1024 * 1024)


def unit_of(rows):
    values = rows.astype(jnp.float32)
    inverse = lax.rsqrt(jnp.mean(values * values, axis=1, keepdims=True) + 1e-06)
    return (values * inverse * (1.0 / math.sqrt(rows.shape[1]))).astype(jnp.bfloat16)


def tag_kernel(
    rows_hbm, label_hbm, whole_ref, head_ref, tail_ref, low_ref, mark_ref, rows_ref, label_ref, done
):
    rows, width = rows_ref.shape
    cut = head_ref.shape[0] - TAG_ROWS
    spans = [(low, low + rows // 4) for low in range(0, rows, rows // 4)]
    labels = pltpu.make_async_copy(label_hbm, label_ref, done.at[len(spans)])
    labels.start()
    copies = []
    for at, (low, high) in enumerate(spans):
        part = pl.ds(low, high - low)
        copies.append(pltpu.make_async_copy(rows_hbm.at[part], rows_ref.at[part], done.at[at]))
        copies[-1].start()
    labels.wait()
    codes = (label_ref[...] + 1).astype(jnp.float32)
    line = jnp.broadcast_to(codes, (TAG_ROWS, rows)).astype(jnp.bfloat16)
    mark_ref[...] = line
    for ref, count in ((whole_ref, rows), (head_ref, cut), (low_ref, rows - cut)):
        ref[count:, :rows] = line
        if rows < width:
            ref[count:, rows:] = jnp.zeros((TAG_ROWS, width - rows), jnp.bfloat16)
    for copy, (low, high) in zip(copies, spans):
        copy.wait()
        unit = unit_of(rows_ref[low:high, :])
        whole_ref[low:high, :] = unit
        if high <= cut:
            head_ref[low:high, :] = unit
        else:
            tail_ref[low - cut : high - cut, :] = unit
            low_ref[low - cut : high - cut, :] = unit


def tagged(embeddings, labels):
    rows, width = embeddings.shape
    labels = labels.reshape(1, rows)
    cut = rows // 2
    shapes = ((rows + TAG_ROWS, width), (cut + TAG_ROWS, width), (rows - cut, width))
    shapes += ((rows - cut + TAG_ROWS, width), (TAG_ROWS, rows))
    return pl.pallas_call(
        tag_kernel,
        out_shape=[pltpu.VMEM(shape, jnp.bfloat16) for shape in shapes],
        in_specs=[pl.BlockSpec(memory_space=pltpu.HBM)] * 2,
        scratch_shapes=[
            pltpu.VMEM((rows, width), jnp.bfloat16),
            pltpu.VMEM((1, rows), jnp.int32),
            pltpu.SemaphoreType.DMA((5,)),
        ],
        compiler_params=PARAMS,
        name="tagged",
    )(*[pltpu.with_memory_space_constraint(value, pltpu.HBM) for value in (embeddings, labels)])


def ridge_kernel(rows_ref, mark_ref, out_ref):
    rows, width = rows_ref.shape
    out_ref[:rows, :] = unit_of(rows_ref[...])
    out_ref[rows:, :rows] = mark_ref[...]
    if rows < width:
        out_ref[rows:, rows:] = jnp.zeros((TAG_ROWS, width - rows), jnp.bfloat16)


def arrived(rows, marks):
    count, width = rows.shape
    return pl.pallas_call(
        ridge_kernel,
        out_shape=pltpu.VMEM((count + TAG_ROWS, width), jnp.bfloat16),
        in_specs=[pl.BlockSpec(memory_space=pltpu.VMEM)] * 2,
        compiler_params=PARAMS,
        name="arrived",
    )(*[pltpu.with_memory_space_constraint(value, pltpu.VMEM) for value in (rows, marks)])


class Block:
    def __init__(self, rows_ref, tag_ref, low, count):
        self.rows_ref = rows_ref
        self.tag_ref = tag_ref
        self.low = low
        self.count = count

    def rows(self):
        return self.rows_ref[: self.count, :]

    def codes(self):
        tags = self.tag_ref[self.tag_ref.shape[0] - TAG_ROWS :, self.low : self.low + self.count]
        return tags.astype(jnp.float32)[:1]

    def columns(self):
        return jnp.transpose(jnp.broadcast_to(self.codes(), (LANES, self.count)))


def whole(ref):
    return [Block(ref, ref, 0, ref.shape[0] - TAG_ROWS)]


def split(head_ref, tail_ref):
    cut = head_ref.shape[0] - TAG_ROWS
    return [
        Block(head_ref, head_ref, 0, cut),
        Block(tail_ref, head_ref, cut, tail_ref.shape[0]),
    ]


def paired(head_ref, low_ref):
    cut = head_ref.shape[0] - TAG_ROWS
    count = low_ref.shape[0] - TAG_ROWS
    return [Block(head_ref, head_ref, 0, cut), Block(low_ref, low_ref, cut, count)]


def halves(upper_ref, lower_ref):
    count = upper_ref.shape[0]
    return [Block(upper_ref, lower_ref, 0, count), Block(lower_ref, lower_ref, count, count)]


def raise_best(out_ref, low, query, keys, switch=None, before=False):
    codes = query.codes()
    if switch is not None:
        codes = jnp.where(switch, codes, -1.0)
    queries = query.rows()
    best = [None] * (query.count // LANES)
    merged = len(keys) > 1 and all(key.count < 2 * LANES for key in keys)
    pieces = [keys] if merged else [[key] for key in keys]
    for piece in pieces:
        rows = jnp.concatenate([key.rows() for key in piece], axis=0) if merged else piece[0].rows()
        columns = [key.columns() for key in piece]
        columns = jnp.concatenate(columns, axis=0) if merged else columns[0]
        count = rows.shape[0]
        scores = lax.dot_general(
            rows, queries, (((1,), (1,)), ((), ())), preferred_element_type=jnp.float32
        )
        for b in range(query.count // LANES):
            span = slice(b * LANES, (b + 1) * LANES)
            allowed = columns == codes[:, span]
            if before:
                key_at = lax.broadcasted_iota(jnp.int32, (count, LANES), 0)
                query_at = lax.broadcasted_iota(jnp.int32, (count, LANES), 1) + b * LANES
                allowed = allowed & (key_at < query_at)
            kept = jnp.where(allowed, scores[:, span], -1.0)
            part = jnp.max(kept.reshape(count // 8, 8, LANES), axis=0)
            best[b] = part if best[b] is None else jnp.maximum(best[b], part)
    for b, part in enumerate(best):
        span = slice(low + b * LANES, low + (b + 1) * LANES)
        line = jnp.max(part, axis=0, keepdims=True)
        out_ref[:, span] = jnp.maximum(out_ref[:, span], line)


def raise_all(outs, queries, keys):
    for out_ref, blocks in zip(outs, queries):
        for block in blocks:
            raise_best(out_ref, block.low, block, keys)


def finish_kernel(*refs):
    refs[-1][...] = functools.reduce(jnp.maximum, [ref[...] for ref in refs[:-1]])


def place():
    index = lax.axis_index("wide")
    return index // 4, (index // 2) % 2, index % 2


def own_kernel(mine_ref, twin_ref, out_ref):
    core = place()[2]
    out_ref[...] = jnp.full(out_ref.shape, -1.0, jnp.float32)
    mine = whole(mine_ref)[0]
    raise_best(out_ref, 0, mine, whole(mine_ref), before=True)

    @pl.when(core == 1)
    def _():
        raise_best(out_ref, 0, mine, whole(twin_ref))


def here_kernel(
    own_ref, mine_ref, twin_ref, side_ref, side_low_ref, ridge_ref, ridge_twin_ref,
    head_ref, tail_ref, mine_out, side_out, above_out,
):
    layer, column, _ = place()
    mine_out[...] = own_ref[...]
    for ref in (side_out, above_out):
        ref[...] = jnp.full(ref.shape, -1.0, jnp.float32)
    near = [whole(mine_ref), paired(side_ref, side_low_ref)]

    @pl.when(column == 0)
    def _():
        raise_all([side_out], near[1:], whole(mine_ref) + whole(twin_ref))

    @pl.when(layer == 2)
    def _():
        keys = whole(ridge_ref) + whole(ridge_twin_ref)
        above = split(head_ref, tail_ref)
        raise_all([mine_out, side_out, above_out], near + [above], keys)


VIEWS = {
    "whole": whole,
    "split": split,
    "halves": halves,
    "paired": paired,
    "end": lambda head_ref, tail_ref: split(head_ref, tail_ref)[1:],
    "first": lambda head_ref, spare_ref: whole(head_ref),
    "low": lambda upper_ref, lower_ref: halves(upper_ref, lower_ref)[1:],
}


def seen(views, refs):
    listed = []
    for view, count in views:
        listed.append(VIEWS[view](*refs[:count]))
        refs = refs[count:]
    return listed, refs


def deep_kernel(queries, keys, started, worker, *refs):
    layer = place()[0]
    begun, refs = (refs[: len(queries)], refs[len(queries) :]) if started else ((), refs)
    query_blocks, refs = seen(queries, refs)
    key_blocks, outs = seen(keys, refs)
    for at, ref in enumerate(outs):
        ref[...] = begun[at][...] if started else jnp.full(ref.shape, -1.0, jnp.float32)

    @pl.when((layer == worker) if worker else (layer % 2 == 1))
    def _():
        raise_all(outs, query_blocks, [block for blocks in key_blocks for block in blocks])


def scored(body, outputs, pairs, *arrays):
    width = arrays[-1].shape[1]
    return pl.pallas_call(
        body,
        out_shape=[pltpu.VMEM((1, count), jnp.float32) for count in outputs],
        in_specs=[pl.BlockSpec(memory_space=pltpu.VMEM)] * len(arrays),
        cost_estimate=pl.CostEstimate(
            flops=2 * pairs * width,
            transcendentals=0,
            bytes_accessed=sum(value.nbytes for value in arrays),
        ),
        compiler_params=PARAMS,
    )(*[pltpu.with_memory_space_constraint(value, pltpu.VMEM) for value in arrays])


def deepened(begun, queries, keys, worker=2):
    def views(blocks):
        return tuple((view, len(arrays)) for view, *arrays in blocks)

    rows = [sum(value.shape[0] for value in arrays) // LANES * LANES for _, *arrays in queries]
    ends = [arrays[-1].shape[0] // LANES * LANES for _, *arrays in keys]
    started = begun is not None
    body = functools.partial(deep_kernel, views(queries), views(keys), started, worker)
    arrays = [value for _, *values in (*queries, *keys) for value in values]
    pairs = sum(rows) * sum(ends)
    return scored(body, rows, pairs, *(begun if started else ()), *arrays)


def layered(embeddings, cluster_id):
    rows = embeddings.shape[0]
    spots = [(z, x, c) for z in range(LAYERS) for x in range(2) for c in range(2)]

    def hops(move):
        def at(z, x, c):
            return (z * 2 + x) * 2 + c

        return [(at(*spot), at(*move(*spot))) for spot in spots]

    across = hops(lambda z, x, c: (z, 1 - x, c))
    beside = hops(lambda z, x, c: (z, x, 1 - c))
    outer = hops(lambda z, x, c: (z ^ 1, x, c))
    inner = hops(lambda z, x, c: (z, x, 1 - c) if z in (0, 3) else (3 - z, x, c))
    slant = hops(lambda z, x, c: (z ^ 1, 1 - x, c))
    spring = hops(lambda z, x, c: ((z, x, 1 - c), (3, x, c), (1, x, c), (2, x, c))[z])

    def sent(value, pairs):
        return lax.ppermute(value, "wide", pairs)

    raw_ridge = sent(embeddings, inner)
    mine, head, tail, low, marks = tagged(embeddings, cluster_id[:, 0])
    near_head = sent(head, outer)
    side_low = sent(low, across)
    near_tail = sent(tail, outer)
    side = sent(head, across)
    twin = sent(mine, beside)
    ridge = arrived(raw_ridge, sent(marks, inner))
    deep_head = sent(near_head, inner)
    upper = sent(near_head[: rows // 2], across)
    lower = sent(side_low, outer)
    near_head_twin = sent(near_head, beside)
    deep_tail = sent(near_tail, inner)
    near_tail_twin = sent(near_tail, beside)
    ridge_twin = sent(ridge, beside)
    deep_head_twin = sent(deep_head, beside)
    lower_twin = sent(lower, beside)

    square = rows * rows
    (own,) = scored(own_kernel, [rows], 2 * square, mine, twin)
    best = scored(
        here_kernel, [rows] * 3, 8 * square,
        own, mine, twin, side, side_low, ridge, ridge_twin, near_head, near_tail,
    )
    flat = [("whole", mine), ("paired", side, side_low)]
    steep = [("split", near_head, near_tail), ("halves", upper, lower)]
    layers = [("split", near_head, near_tail), ("split", near_head_twin, near_tail_twin)]
    best = deepened(best[:2], flat, layers, worker=None) + best[2:]
    deep, deep_twin = ("whole", deep_head), ("whole", deep_head_twin)
    best = deepened(best, flat + steep[:1], [deep])
    best = deepened(best, flat + steep[:1], [deep_twin])
    keys = [("whole", ridge), ("whole", ridge_twin), deep, deep_twin]
    first, second = best[:2]
    from_side = sent(second, across)
    third, fourth = best[2:] + deepened(None, steep[1:], keys)
    from_below = sent(third, outer)
    from_far = sent(fourth, slant)
    ends = [
        ("end", near_head, near_tail), ("end", near_head_twin, near_tail_twin),
        ("low", upper, lower), ("low", upper, lower_twin),
    ]
    guests = [("whole", ridge), ("first", deep_head, near_tail)]
    begun = deepened(None, guests, ends[:2], worker=1)
    lent, lifted = deepened(begun, guests, ends[2:], worker=1)
    (lifted,) = deepened([lifted], [("end", deep_head, deep_tail)], ends, worker=1)
    from_lifted = sent(lifted, spring)
    from_lent = sent(lent, inner)
    parts = (first, from_side, from_below, from_far, from_lent, from_lifted)
    (best,) = pl.pallas_call(
        finish_kernel,
        out_shape=[jax.ShapeDtypeStruct((1, rows), jnp.float32)],
        in_specs=[pl.BlockSpec(memory_space=pltpu.VMEM)] * len(parts),
        compiler_params=PARAMS,
        name="finish",
    )(*[pltpu.with_memory_space_constraint(value, pltpu.VMEM) for value in parts])
    return best.reshape(rows)


def per_device(embeddings, cluster_id):
    if lax.axis_size("wide") == 4 * LAYERS:
        return layered(embeddings, cluster_id)
    return routed(embeddings, cluster_id)


def solution(mesh):
    placed = (P(("dom", "wide"), None), P(("dom", "wide"), None))
    return jax.shard_map(
        per_device, mesh=mesh, in_specs=placed, out_specs=P(("dom", "wide")), check_vma=False
    )
```
